32 devices in a mesh: dp: 4 (over x, y), sp: 8 (over z, core).
Axes of the slice: x: 2, y: 2, z: 4, core: 2. Of those that a mesh axis runs over, the one named last changes fastest.
Arguments:
- x: bfloat16 [16384, 4096], P(('dp', 'sp')), parts along dimension 0
- gain: bfloat16 [4096], replicated
- wq: bfloat16 [4096, 4096], P('sp')
- wk: bfloat16 [4096, 256], P('sp')
- wv: bfloat16 [4096, 256], P('sp')
- wo: bfloat16 [4096, 4096], P('sp')
Outputs:
- output: bfloat16 [16384, 4096], P(('dp', 'sp')), parts along dimension 0
There are 4 independent parts. The reference program is written for one: setup_inputs(seed, part) draws one part's arguments, and reference() takes and returns one part's arrays. A program takes and returns all parts, laid end to end along the dimension named above; an argument that names none is the same for every part.
All inputs are finite; a program needn't handle non-finite values.
Results may differ from the reference program's by a relative error of at most 0.012.
Values are sent between devices in bfloat16 or wider.
A program may use at most 2 GiB of HBM per device.

```python
import jax
import jax.numpy as jnp
from jax import lax

ROWS = 4096
D = 4096
HEADS = 16
KV_HEADS = 1
HEAD = 256
THETA = 10000


def setup_inputs(seed: int = 0, part: int = 0) -> dict:
    kx, kn, kq, kk, kv, ko = jax.random.split(jax.random.key(seed), 6)

    def weights(key, rows, columns):
        return jax.random.normal(key, (rows, columns), jnp.float32) * rows**-0.5

    drawn = {
        "x": jax.random.normal(jax.random.fold_in(kx, part), (ROWS, D), jnp.float32),
        "gain": 1 + 0.1 * jax.random.normal(kn, (D,), jnp.float32),
        "wq": 2 * weights(kq, D, HEADS * HEAD),
        "wk": 2 * weights(kk, D, KV_HEADS * HEAD),
        "wv": 4 * weights(kv, D, KV_HEADS * HEAD),
        "wo": weights(ko, HEADS * HEAD, D),
    }
    return {k: v.astype(jnp.bfloat16) for k, v in drawn.items()}


def normed(x, gain):
    wide = x.astype(jnp.float32)
    scale = lax.rsqrt(jnp.mean(wide * wide, -1, keepdims=True) + 1e-6)
    return (wide * scale * gain.astype(jnp.float32)).astype(jnp.bfloat16)


def turned(t, place, theta):
    half = t.shape[-1] // 2
    angle = place.astype(jnp.float32)[:, None] * theta ** (-jnp.arange(half, dtype=jnp.float32) / half)
    cos, sin = jnp.cos(angle)[:, None], jnp.sin(angle)[:, None]
    a, b = t[..., :half].astype(jnp.float32), t[..., half:].astype(jnp.float32)
    return jnp.concatenate([a * cos - b * sin, b * cos + a * sin], -1).astype(jnp.bfloat16)


def matmul(a, w):
    return jnp.dot(a, w, preferred_element_type=jnp.float32).astype(jnp.bfloat16)


def einsum(form, a, b):
    return jnp.einsum(form, a.astype(jnp.float32), b.astype(jnp.float32))


def attention(q, k, v):
    scores = einsum("tgsd,ugd->gstu", q, k) * q.shape[-1] ** -0.5
    token = jnp.arange(q.shape[0])
    scores = jnp.where(token[:, None] >= token, scores, -jnp.inf)
    weights = jax.nn.softmax(scores, -1).astype(jnp.bfloat16)
    return einsum("gstu,ugd->tgsd", weights, v).astype(jnp.bfloat16)


def reference(x, gain, wq, wk, wv, wo):
    a, place = normed(x, gain), jnp.arange(ROWS)
    q = turned(matmul(a, wq).reshape(ROWS, HEADS, HEAD), place, THETA).reshape(ROWS, KV_HEADS, -1, HEAD)
    k = turned(matmul(a, wk).reshape(ROWS, KV_HEADS, HEAD), place, THETA)
    v = matmul(a, wv).reshape(ROWS, KV_HEADS, HEAD)
    seen = attention(q, k, v).reshape(ROWS, HEADS * HEAD)
    return (x.astype(jnp.float32) + jnp.dot(seen, wo, preferred_element_type=jnp.float32)).astype(jnp.bfloat16)
```

```python
import functools

import jax
import jax.numpy as jnp
from jax import lax
from jax.experimental import pallas as pl
from jax.experimental.pallas import tpu as pltpu
from jax.sharding import PartitionSpec as P

MESH = pl.DeviceIdType.MESH
HEAD = 256
HEADS = 16
THETA = 10000
NEG = -1e30
HIDDEN = 2 * NEG
LOG2E = 1.4426950408889634
OWN = 512
D = 4096
CHUNKS = 4
KV = 2 * CHUNKS
GROUP = 2
COMPUTE = True


def _dot(a, b, ca, cb):
    return lax.dot_general(a, b, (((ca,), (cb,)), ((), ())), preferred_element_type=jnp.float32)


def _turn(t, cos, sin):
    a, b = t[:, : HEAD // 2], t[:, HEAD // 2 :]
    return jnp.concatenate([a * cos - b * sin, b * cos + a * sin], axis=1).astype(jnp.bfloat16)


def _kernel(x_hbm, gain_ref, wq, wk, wv, wo, cos_ref, sin_ref, y_hbm, w_all,
            kv_all, xv, lhs, qs, ks, vts, acc, wt, top_s, mix_s,
            recv_z, recv_x, recv_y, recv_xh, recv_yh, recv_d,
            s_up, s_dn, s_x, s_y, s_xh, s_yh, s_d,
            r_kv, r_kvd, s_kv, s_kvd, l_sem, x_sem, y_sem, o_sem):
    p, sp = lax.axis_index("dp"), lax.axis_index("sp")
    z, r = lax.div(sp, 2), lax.rem(sp, 2)
    other = 1 - r
    px, py, pd = lax.rem(p + 2, 4), p + 1 - 2 * lax.rem(p, 2), 3 - p
    hi = lax.div(z, 2)
    u = z + hi * (3 - 2 * z)
    step = 2 * (1 - 2 * hi)
    DEV_IN, DEV_OUT = (p, sp + step), (p, sp - step)
    DEV_X, DEV_Y, DEV_D = (px, sp), (py, sp), (p, sp + 1 - 2 * r)
    inner, outer = u == 1, u == 0

    def source(k):
        su = k - u if k == 1 else k
        return su + hi * (3 - 2 * su)

    def send(src, dst, ssem, rsem, dev):
        pltpu.make_async_remote_copy(src_ref=src, dst_ref=dst, send_sem=ssem, recv_sem=rsem, device_id=dev, device_id_type=MESH).start()

    def got(ref, sem):
        pltpu.make_async_copy(ref, ref, sem).wait()

    def piece(t, s, rr, q, half=None):
        if t == KV if isinstance(t, int) else False:
            ref = kv_all.at[s, rr, q]
            n = 128
        else:
            ref = w_all.at[t, s, rr, q]
            n = 256
        return ref if half is None else ref.at[pl.ds(half * n, n)]

    def own_kv(q):
        return (wk, wv)[q % 2].at[pl.ds((q // 2) * 256, 256)]

    def columns(ref, q, c):
        return ref.at[:, pl.ds(pl.multiple_of((q * CHUNKS + c) * HEAD, HEAD), HEAD)]

    def send_own_z(t, src):
        send(src, piece(t, z, r, p), s_up.at[t], recv_z.at[t, z], DEV_IN)

        @pl.when(inner)
        def _():
            send(src, piece(t, z, r, p), s_dn.at[t], recv_z.at[t, z], DEV_OUT)

    def send_own_kv():
        for odd in range(2):
            @pl.when(lax.rem(p, 2) == odd)
            def _():
                src = (wk, wv)[odd].at[pl.ds(pl.multiple_of(lax.div(p, 2) * 256, 256), 256)]
                send_own_z(KV, src)
        for q in range(4):
            send(own_kv(q), piece(KV, z, r, q), s_d.at[KV], recv_d.at[KV, z], DEV_D)

    def send_own(t):
        def go(ref, c):
            send_own_z(t, columns(ref, p, c))
            for q in range(4):
                send(columns(ref, q, c), piece(t, z, r, q), s_d.at[t], recv_d.at[t, z], DEV_D)

        @pl.when(t < CHUNKS)
        def _():
            go(wq, t)

        @pl.when(t >= CHUNKS)
        def _():
            go(wo, t - CHUNKS)

    def hand(t, s, q, half=None):
        send(piece(t, s, r, q, half), piece(t, s, r, q, half), s_d.at[t], recv_d.at[t, s], DEV_D)

    def stage1(t, k):
        s = source(k)
        mine = piece(t, s, r, p)
        got(mine, recv_z.at[t, s])

        @pl.when(inner)
        def _():
            if k == 1:
                send(mine, mine, s_up.at[t], recv_z.at[t, s], DEV_IN)
            else:
                send(mine, mine, s_dn.at[t], recv_z.at[t, s], DEV_OUT)

        send(mine, mine, s_x.at[t], recv_x.at[t, s], DEV_X)
        send(mine, mine, s_y.at[t], recv_y.at[t, s], DEV_Y)
        hand(t, s, p)

    def stage2(t, k):
        s = source(k)
        got(piece(t, s, r, px), recv_x.at[t, s])
        part = piece(t, s, r, px, 0)
        send(part, part, s_yh.at[t], recv_yh.at[t, s], DEV_Y)
        hand(t, s, px)
        got(piece(t, s, r, py), recv_y.at[t, s])
        part = piece(t, s, r, py, 1)
        send(part, part, s_xh.at[t], recv_xh.at[t, s], DEV_X)
        hand(t, s, py)

    def stage3(t, k):
        s = source(k)
        got(piece(t, s, r, pd, 0), recv_yh.at[t, s])
        hand(t, s, pd, 0)
        got(piece(t, s, r, pd, 1), recv_xh.at[t, s])
        hand(t, s, pd, 1)

    def handed(t, s):
        ref = kv_all if isinstance(t, int) and t == KV else w_all.at[t]
        got(ref.at[s, other], recv_d.at[t, s])

    def sent(t):
        kv = isinstance(t, int) and t == KV
        ref = kv_all if kv else w_all.at[t]
        n = 128 if kv else 256

        @pl.when(outer)
        def _():
            got(ref.at[0, 0, 0], s_up.at[t])

        @pl.when(inner)
        def _():
            got(ref.at[0, 0, pl.ds(0, 2)], s_up.at[t])
            got(ref.at[0, 0, pl.ds(0, 3)], s_dn.at[t])

        got(ref.at[0, 0, pl.ds(0, 3)], s_x.at[t])
        got(ref.at[0, 0, pl.ds(0, 3)], s_y.at[t])
        got(ref.at[0, 0, pl.ds(0, 3), pl.ds(0, n)], s_xh.at[t])
        got(ref.at[0, 0, pl.ds(0, 3), pl.ds(0, n)], s_yh.at[t])
        got(ref.at[pl.ds(0, 2)], s_d.at[t])

    def kv_send(s, up):
        i = 2 * s + r
        k_ref, v_ref = ks.at[i], vts.at[i, pl.ds(0, HEAD)]
        send(k_ref, k_ref, s_kvd.at[0, s], r_kvd.at[0, s], DEV_D)
        send(v_ref, v_ref, s_kvd.at[1, s], r_kvd.at[1, s], DEV_D)
        if up:
            @pl.when(z < 3)
            def _():
                send(k_ref, k_ref, s_kv.at[0, s], r_kv.at[0, s], (p, sp + 2))
                send(v_ref, v_ref, s_kv.at[1, s], r_kv.at[1, s], (p, sp + 2))

    def kv_take(j):
        @pl.when(z >= j)
        def _():
            s = z - j
            got(ks.at[2 * s + r], r_kv.at[0, s])
            got(vts.at[2 * s + r, pl.ds(0, HEAD)], r_kv.at[1, s])
            kv_send(s, True)

    def kv_handed():
        for j in range(4):
            @pl.when(z >= j)
            def _():
                s = z - j
                got(ks.at[2 * s + other], r_kvd.at[0, s])
                got(vts.at[2 * s + other, pl.ds(0, HEAD)], r_kvd.at[1, s])

    def kv_sent():
        for j in range(4):
            @pl.when(z >= j)
            def _():
                s = z - j
                for i in range(2):
                    got(ks.at[0], s_kvd.at[i, s])

                    @pl.when(z < 3)
                    def _():
                        got(ks.at[0], s_kv.at[i, s])

    def norm(i):
        def rows(n, _):
            at = pl.ds(pl.multiple_of(i * 128 + n * 32, 32), 32)
            wide = xv[at, :].astype(jnp.float32)
            scale = lax.rsqrt(jnp.mean(wide * wide, axis=-1, keepdims=True) + 1e-6)
            out = (wide * scale * gain_ref[...].astype(jnp.float32)).astype(jnp.bfloat16)
            for h in range(HEADS):
                lhs[0, h, at, :] = out[:, h * HEAD : (h + 1) * HEAD]

        lax.fori_loop(0, 4, rows, None)

    def kv_project():
        for q in range(4):
            pltpu.make_async_copy(own_kv(q), kv_all.at[z, r, q], l_sem.at[0]).start()
        got(kv_all.at[z, r], l_sem.at[0])
        for k in range(4):
            handed(KV, z if k == 0 else source(k))

        for which in range(2):
            def one(n, total):
                for half in range(2):
                    w = kv_all[lax.div(n, 2), lax.rem(n, 2), 2 * half + which]
                    total += _dot(lhs[0, 2 * n + half], w, 1, 0)
                return total

            acc[which] = jnp.zeros((OWN, HEAD), jnp.float32)

            def loop(n, _):
                acc[which] = one(n, acc[which])

            lax.fori_loop(0, 8, loop, None)
        k = acc[0].astype(jnp.bfloat16).astype(jnp.float32)
        ks[sp] = _turn(k, cos_ref[...], sin_ref[...])
        vts[sp, pl.ds(0, HEAD), :] = acc[1].T.astype(jnp.bfloat16)
        for i in range(8):
            vts[i, pl.ds(HEAD, 16), :] = jnp.ones((16, OWN), jnp.bfloat16)

    def load(t, k):
        b = k % 2
        if k:
            s = source(k)
            handed(t, s)
            pltpu.make_async_copy(w_all.at[t, s], wt.at[b], l_sem.at[b]).start()
        else:
            handed(t, z)
            pltpu.make_async_copy(w_all.at[t, z, other], wt.at[b, other], l_sem.at[b]).start()

            def go(ref, c):
                for q in range(4):
                    pltpu.make_async_copy(columns(ref, q, c), wt.at[b, r, q], l_sem.at[b]).start()

            @pl.when(t < CHUNKS)
            def _():
                go(wq, t)

            @pl.when(t >= CHUNKS)
            def _():
                go(wo, t - CHUNKS)

    def mm(t, k):
        b = k % 2
        got(wt.at[b], l_sem.at[b])
        s = source(k) if k else z
        m = lax.div(t, CHUNKS)

        def one(q, _):
            total = None
            for rr in range(2):
                for half in range(2):
                    d = _dot(lhs[m, 4 * s + 2 * rr + half], wt[b, rr, q, pl.ds(half * 256, 256), :], 1, 0)
                    total = d if total is None else total + d
            acc[q] = total if k == 0 else acc[q] + total

        lax.fori_loop(0, 4, one, None)

    def finish(t):
        @pl.when(t < CHUNKS)
        def _():
            def one(q, _):
                v = acc[q].astype(jnp.bfloat16).astype(jnp.float32)
                qs[q * CHUNKS + t] = _turn(v, cos_ref[...], sin_ref[...])

            lax.fori_loop(0, 4, one, None)

        @pl.when(t >= CHUNKS)
        def _():
            def one(q, _):
                at = pl.ds(pl.multiple_of((q * CHUNKS + t - CHUNKS) * HEAD, HEAD), HEAD)
                xv[:, at] = (xv[:, at].astype(jnp.float32) + acc[q]).astype(jnp.bfloat16)
                pltpu.make_async_copy(xv.at[:, at], y_hbm.at[:, at], y_sem.at[t - CHUNKS]).start()

            lax.fori_loop(0, 4, one, None)

    def attend(n):
        e = HEAD**-0.5 * LOG2E
        heads = []
        for i in range(GROUP):
            at = n * GROUP + i
            heads.append(lax.rem(at, 4) * CHUNKS + lax.div(at, 4))
        for i in range(GROUP):
            top_s[i] = jnp.full((1, OWN), NEG, jnp.float32)
            mix_s[i] = jnp.zeros((HEAD + 8, OWN), jnp.float32)

        def block(j, masked):
            keys = ks[j]
            scores = [_dot(keys, qs[h], 1, 1) for h in heads]
            weights, keeps = [], []
            for i, s in enumerate(scores):
                if masked:
                    ok = lax.broadcasted_iota(jnp.int32, (OWN, OWN), 1) >= lax.broadcasted_iota(jnp.int32, (OWN, OWN), 0)
                    s = jnp.where(ok, s, HIDDEN)
                old = top_s[i]
                top = jnp.maximum(old, s.max(axis=0, keepdims=True))
                top_s[i] = top
                weights.append(jnp.exp2((s - top) * e).astype(jnp.bfloat16))
                keeps.append(jnp.exp2((old - top) * e))
            values = vts[j, pl.ds(0, HEAD + 8), :]
            for i, (w, keep) in enumerate(zip(weights, keeps)):
                mix_s[i] = mix_s[i] * keep + _dot(values, w, 1, 0)

        lax.fori_loop(0, sp, lambda j, _: block(j, False), None)
        block(sp, True)
        for i, h in enumerate(heads):
            lhs[1, h] = (mix_s[i, pl.ds(0, HEAD), :] * (1 / mix_s[i, pl.ds(HEAD, 1), :])).T.astype(jnp.bfloat16)

    barrier = pltpu.get_barrier_semaphore()
    for dev in (DEV_IN, DEV_X, DEV_Y, DEV_D):
        pl.semaphore_signal(barrier, inc=1, device_id=dev, device_id_type=MESH)

    @pl.when(inner)
    def _():
        pl.semaphore_signal(barrier, inc=1, device_id=DEV_OUT, device_id_type=MESH)

    if COMPUTE:
        pltpu.make_async_copy(x_hbm, xv, x_sem.at[0]).start()

    @pl.when(inner)
    def _():
        pl.semaphore_wait(barrier, 5)

    @pl.when(outer)
    def _():
        pl.semaphore_wait(barrier, 4)

    send_own_kv()
    send_own(0)
    if COMPUTE:
        got(xv, x_sem.at[0])
        norm(0)
    stage1(KV, 1)
    if COMPUTE:
        norm(1)
    stage1(KV, 2)
    stage2(KV, 1)
    if COMPUTE:
        norm(2)
    stage1(KV, 3)
    stage2(KV, 2)
    stage3(KV, 1)
    if COMPUTE:
        norm(3)
    stage2(KV, 3)
    stage3(KV, 2)
    stage3(KV, 3)

    def attend_slots(t, slot):
        per = {4: ((0,), (1,), (2,)), 5: ((3,), (4,), (5,)), 6: ((6,), (7,), ())}
        for tt, slots in per.items():
            if slots[slot]:
                @pl.when(t == tt)
                def _():
                    for n in slots[slot]:
                        attend(n)

    def multiply_a(t):
        load(t, 0)
        load(t, 1)

    def multiply_b(t):
        mm(t, 0)
        mm(t, 1)
        load(t, 2)

    def multiply_c(t):
        load(t, 3)
        mm(t, 2)

    def multiply_d(t):
        mm(t, 3)
        finish(t)

    def work(t, slot):
        pass

    def round_(t, _):
        @pl.when(t < 2 * CHUNKS - 1)
        def _():
            send_own(t + 1)

        before = t - 1
        first = t == 0
        early = (t >= 1) & (t <= CHUNKS)
        if COMPUTE:
            @pl.when(early)
            def _():
                multiply_a(before)

        stage1(t, 1)

        @pl.when(t > 0)
        def _():
            stage2(before, 3)
            stage3(before, 2)

        if COMPUTE:
            @pl.when(first)
            def _():
                kv_project()

            @pl.when(early)
            def _():
                multiply_b(before)

            at = jnp.clip(t - 4, 0, 2) * 3

            @pl.when((t >= 4) & (t <= 6))
            def _():
                @pl.when(t == 4)
                def _():
                    kv_handed()
                attend((t - 4) * 3)

        stage1(t, 2)
        stage2(t, 1)

        @pl.when(t > 0)
        def _():
            stage3(before, 3)

        if COMPUTE:
            @pl.when(first)
            def _():
                kv_send(z, True)

            @pl.when(early)
            def _():
                multiply_c(before)

            @pl.when((t >= 4) & (t <= 6))
            def _():
                attend((t - 4) * 3 + 1)

        stage1(t, 3)
        stage2(t, 2)
        stage3(t, 1)
        if COMPUTE:
            for j in range(1, 4):
                @pl.when(t == j)
                def _():
                    kv_take(j)

            @pl.when(early)
            def _():
                multiply_d(before)

            @pl.when((t >= 4) & (t <= 5))
            def _():
                attend((t - 4) * 3 + 2)

            @pl.when(t == 6)
            def _():
                for part in (multiply_a, multiply_b, multiply_c, multiply_d):
                    part(4)

            @pl.when(t == 7)
            def _():
                def late(n, _):
                    for part in (multiply_a, multiply_b, multiply_c, multiply_d):
                        part(n)
                lax.fori_loop(5, 7, late, None)

    lax.fori_loop(0, 2 * CHUNKS, round_, None)
    last = 2 * CHUNKS - 1
    stage2(last, 3)
    stage3(last, 2)
    if COMPUTE:
        load(last, 0)
        load(last, 1)
        mm(last, 0)
        mm(last, 1)
        load(last, 2)
    stage3(last, 3)
    if COMPUTE:
        mm(last, 2)
        load(last, 3)
        mm(last, 3)
        finish(last)
    else:
        handed(KV, z)
        for k in range(1, 4):
            handed(KV, source(k))
        def hh(t, _):
            handed(t, z)
            for k in range(1, 4):
                handed(t, source(k))
        lax.fori_loop(0, 8, hh, None)
    sent(KV)
    lax.fori_loop(0, 2 * CHUNKS, lambda t, _: sent(t), None)
    if COMPUTE:
        kv_sent()
        for c in range(CHUNKS):
            got(y_hbm.at[:, pl.ds(0, 4 * HEAD)], y_sem.at[c])


def solution(mesh):
    bf, f32 = jnp.bfloat16, jnp.float32
    any_, vmem = pl.BlockSpec(memory_space=pl.ANY), pl.BlockSpec(memory_space=pltpu.VMEM)
    dma = pltpu.SemaphoreType.DMA

    def step(x, gain, wq, wk, wv, wo):
        half = HEAD // 2
        place = lax.axis_index("sp") * OWN + jnp.arange(OWN)
        angle = place.astype(f32)[:, None] * THETA ** (-jnp.arange(half, dtype=f32) / half)
        n = KV + 1
        y, _ = pl.pallas_call(
            _kernel,
            in_specs=[any_, vmem, any_, any_, any_, any_, vmem, vmem],
            out_specs=[any_, any_],
            out_shape=[jax.ShapeDtypeStruct((OWN, D), bf), jax.ShapeDtypeStruct((2 * CHUNKS, 4, 2, 4, OWN, HEAD), bf)],
            scratch_shapes=[
                pltpu.VMEM((4, 2, 4, 256, HEAD), bf),
                pltpu.VMEM((OWN, D), bf),
                pltpu.VMEM((2, HEADS, OWN, HEAD), bf),
                pltpu.VMEM((HEADS, OWN, HEAD), bf),
                pltpu.VMEM((8, OWN, HEAD), bf),
                pltpu.VMEM((8, HEAD + 16, OWN), bf),
                pltpu.VMEM((4, OWN, HEAD), f32),
                pltpu.VMEM((2, 2, 4, OWN, HEAD), bf),
                pltpu.VMEM((GROUP, 1, OWN), f32),
                pltpu.VMEM((GROUP, HEAD + 8, OWN), f32),
                *[dma((n, 4))] * 6,
                *[dma((n,))] * 7,
                *[dma((2, 4))] * 4,
                dma((2,)), dma((1,)), dma((CHUNKS,)), dma((1,)),
            ],
            compiler_params=pltpu.CompilerParams(collective_id=0, has_side_effects=True, vmem_limit_bytes=62 * 2**20),
            cost_estimate=pl.CostEstimate(flops=10**11, bytes_accessed=10**8, transcendentals=10**7),
        )(x, gain[None], wq, wk, wv, wo, jnp.cos(angle), jnp.sin(angle))
        return y

    tokens, whole = P(("dp", "sp"), None), P("sp", None)
    return jax.shard_map(
        step,
        mesh=mesh,
        in_specs=(tokens, P(None), whole, whole, whole, whole),
        out_specs=tokens,
        check_vma=False,
    )
```

```python
import functools
import itertools

import jax
import jax.numpy as jnp
import numpy as np
from jax import lax
from jax.experimental import pallas as pl
from jax.experimental.pallas import tpu as pltpu
from jax.sharding import PartitionSpec as P

MESH = pl.DeviceIdType.MESH
HEAD = 256
HEADS = 16
THETA = 10000
NEG = -1e30
HIDDEN = 2 * NEG
LOG2E = 1.4426950408889634
OWN = 512
D = 4096
CHUNKS = 4
KV = 2 * CHUNKS
GROUP = 2
COMPUTE = True
BOTH = 64
A0, A2, A3 = 3, 1, 2


def _dot(a, b, ca, cb):
    return lax.dot_general(a, b, (((ca,), (cb,)), ((), ())), preferred_element_type=jnp.float32)


def _turn(t, cos, sin):
    a, b = t[:, : HEAD // 2], t[:, HEAD // 2 :]
    return jnp.concatenate([a * cos - b * sin, b * cos + a * sin], axis=1).astype(jnp.bfloat16)


def _kernel(x_hbm, gain_ref, wq, wk, wv, wo, rate_ref, y_ref, w_all,
            cos_ref, sin_ref,
            kv_all, xv, lhs, qs, ks, vts, acc, wt, top_s, mix_s,
            recv_z, recv_x, recv_y, recv_xh, recv_yh, recv_d,
            s_up, s_dn, s_x, s_y, s_xh, s_yh, s_d,
            r_kv, r_kvd, s_kv, s_kvd, l_sem, x_sem):
    p, sp = lax.axis_index("dp"), lax.axis_index("sp")
    z, r = lax.div(sp, 2), lax.rem(sp, 2)
    other = 1 - r
    px, py, pd = lax.rem(p + 2, 4), p + 1 - 2 * lax.rem(p, 2), 3 - p
    hi = lax.div(z, 2)
    u = z + hi * (3 - 2 * z)
    step = 2 * (1 - 2 * hi)
    DEV_IN, DEV_OUT = (p, sp + step), (p, sp - step)
    DEV_X, DEV_Y, DEV_D = (px, sp), (py, sp), (p, sp + 1 - 2 * r)
    inner, outer = u == 1, u == 0

    def source(k):
        su = k - u if k == 1 else k
        return su + hi * (3 - 2 * su)

    def send(src, dst, ssem, rsem, dev):
        pltpu.make_async_remote_copy(src_ref=src, dst_ref=dst, send_sem=ssem, recv_sem=rsem, device_id=dev, device_id_type=MESH).start()

    def got(ref, sem):
        pltpu.make_async_copy(ref, ref, sem).wait()

    def piece(t, s, rr, q, low=0, high=None):
        ref, rows = (kv_all.at[s, rr, q], 256) if isinstance(t, int) and t == KV else (w_all.at[t, s, rr, q], OWN)
        high = rows if high is None else high
        return ref if high - low == rows else ref.at[pl.ds(low, high - low)]

    def rows_of(t):
        return 256 if isinstance(t, int) and t == KV else OWN

    def by_kind(fn):
        def call(t, *args):
            if isinstance(t, int):
                fn(t, *args, BOTH if CHUNKS <= t < KV else 0)
            else:
                pl.when(t < CHUNKS)(lambda: fn(t, *args, 0))
                pl.when(t >= CHUNKS)(lambda: fn(t, *args, BOTH))

        return call

    def several(t, n, rows):
        ref = kv_all.at[0, 0] if isinstance(t, int) and t == KV else w_all.at[t, 0, 0]
        return ref.at[pl.ds(0, 4), pl.ds(0, n * rows // 4)]

    def own_kv(q):
        return (wk, wv)[q % 2].at[pl.ds((q // 2) * 256, 256)]

    def columns(ref, q, c):
        return ref.at[:, pl.ds(pl.multiple_of((q * CHUNKS + c) * HEAD, HEAD), HEAD)]

    def send_z(t, s, parts, sem, dev):
        for src, dst in parts:
            send(src, dst, sem.at[t], recv_z.at[t, s], dev)

    def send_own_z(t, parts):
        send_z(t, z, parts, s_up, DEV_IN)
        pl.when(inner)(lambda: send_z(t, z, parts, s_dn, DEV_OUT))

    def send_own_kv():
        for odd in range(2):
            @pl.when(lax.rem(p, 2) == odd)
            def _():
                src = (wk, wv)[odd].at[pl.ds(pl.multiple_of(lax.div(p, 2) * 256, 256), 256)]
                send_own_z(KV, [(src, piece(KV, z, r, p))])
        for q in range(4):
            send(own_kv(q), piece(KV, z, r, q), s_d.at[KV], recv_d.at[KV, z], DEV_D)

    def send_own(t):
        def go(ref, c, b):
            parts = [(columns(ref, p, c), piece(t, z, r, p))]
            if b:
                for low in (0, OWN - b):
                    parts.append((columns(ref, pd, c).at[pl.ds(low, b)], piece(t, z, r, pd, low, low + b)))
            send_own_z(t, parts)
            for q in range(4):
                send(columns(ref, q, c), piece(t, z, r, q), s_d.at[t], recv_d.at[t, z], DEV_D)

        @pl.when(t < CHUNKS)
        def _():
            go(wq, t, 0)

        @pl.when(t >= CHUNKS)
        def _():
            go(wo, t - CHUNKS, BOTH)

    def hand(t, s, *part):
        send(piece(t, s, r, *part), piece(t, s, r, *part), s_d.at[t], recv_d.at[t, s], DEV_D)

    def along_z(t, b):
        n = rows_of(t)
        return [(p, 0, n)] + ([(pd, 0, b), (pd, n - b, n)] if b else [])

    @by_kind
    def stage0(t, k, b):
        s = source(k)
        parts = [(piece(t, s, r, *part),) * 2 for part in along_z(t, b)]

        @pl.when(inner)
        def _():
            got(several(t, 1, rows_of(t) + 2 * b), recv_z.at[t, s])
            send_z(t, s, parts, *((s_up, DEV_IN) if k == 1 else (s_dn, DEV_OUT)))

    @by_kind
    def stage1(t, k, b):
        s, n = source(k), rows_of(t)
        pl.when(outer)(lambda: got(several(t, 1, n + 2 * b), recv_z.at[t, s]))
        for parts, ssem, rsem, dev in (
            ([(p, 0, n - b), (pd, 0, b)], s_x, recv_x, DEV_X),
            ([(p, b, n), (pd, n - b, n)], s_y, recv_y, DEV_Y),
        ):
            for part in parts if b else parts[:1]:
                send(piece(t, s, r, *part), piece(t, s, r, *part), ssem.at[t], rsem.at[t, s], dev)
        for part in along_z(t, b):
            hand(t, s, *part)

    @by_kind
    def stage2(t, k, b):
        s, n = source(k), rows_of(t)
        for first, second, rsem, part, ssem, rsem2, dev in (
            ((px, 0, n - b), (py, 0, b), recv_x, (px, b, n // 2), s_yh, recv_yh, DEV_Y),
            ((py, b, n), (px, n - b, n), recv_y, (py, n // 2, n - b), s_xh, recv_xh, DEV_X),
        ):
            got(several(t, 1, n), rsem.at[t, s])
            send(piece(t, s, r, *part), piece(t, s, r, *part), ssem.at[t], rsem2.at[t, s], dev)
            hand(t, s, *first)
            if b:
                hand(t, s, *second)

    @by_kind
    def stage3(t, k, b):
        s, n = source(k), rows_of(t)
        for part, rsem in (((pd, b, n // 2), recv_yh), ((pd, n // 2, n - b), recv_xh)):
            got(piece(t, s, r, *part), rsem.at[t, s])
            hand(t, s, *part)

    def handed(t, s):
        ref = kv_all if isinstance(t, int) and t == KV else w_all.at[t]
        got(ref.at[s, other], recv_d.at[t, s])

    @by_kind
    def sent(t, b):
        n = rows_of(t)
        pl.when(outer)(lambda: got(several(t, 1, n + 2 * b), s_up.at[t]))

        @pl.when(inner)
        def _():
            got(several(t, 2, n + 2 * b), s_up.at[t])
            got(several(t, 3, n + 2 * b), s_dn.at[t])

        for sem, rows in ((s_x, n), (s_y, n), (s_xh, n // 2 - b), (s_yh, n // 2 - b)):
            got(several(t, 3, rows), sem.at[t])
        ref = kv_all if isinstance(t, int) and t == KV else w_all.at[t]
        got(ref.at[pl.ds(0, 2)], s_d.at[t])

    def kv_send(s, up):
        i = 2 * s + r
        k_ref, v_ref = ks.at[i], vts.at[i, pl.ds(0, HEAD)]
        send(k_ref, k_ref, s_kvd.at[0, s], r_kvd.at[0, s], DEV_D)
        send(v_ref, v_ref, s_kvd.at[1, s], r_kvd.at[1, s], DEV_D)
        if up:
            @pl.when(z < 3)
            def _():
                send(k_ref, k_ref, s_kv.at[0, s], r_kv.at[0, s], (p, sp + 2))
                send(v_ref, v_ref, s_kv.at[1, s], r_kv.at[1, s], (p, sp + 2))

    def kv_take(j):
        @pl.when(z >= j)
        def _():
            s = z - j
            got(ks.at[2 * s + r], r_kv.at[0, s])
            got(vts.at[2 * s + r, pl.ds(0, HEAD)], r_kv.at[1, s])
            kv_send(s, True)

    def kv_handed(which):
        for j in which:
            @pl.when(z >= j)
            def _():
                s = z - j
                got(ks.at[2 * s + other], r_kvd.at[0, s])
                got(vts.at[2 * s + other, pl.ds(0, HEAD)], r_kvd.at[1, s])

    def kv_sent():
        for j in range(4):
            @pl.when(z >= j)
            def _():
                s = z - j
                for i in range(2):
                    got(ks.at[0], s_kvd.at[i, s])

                    @pl.when(z < 3)
                    def _():
                        got(ks.at[0], s_kv.at[i, s])

    def tables():
        place = lax.broadcasted_iota(jnp.int32, (OWN, HEAD // 2), 0) + sp * OWN
        angle = place.astype(jnp.float32) * rate_ref[...]
        cos_ref[...] = jnp.cos(angle)
        sin_ref[...] = jnp.sin(angle)

    def norm(i):
        def rows(n, _):
            at = pl.ds(pl.multiple_of(i * 128 + n * 32, 32), 32)
            wide = xv[at, :].astype(jnp.float32)
            scale = lax.rsqrt(jnp.mean(wide * wide, axis=-1, keepdims=True) + 1e-6)
            out = (wide * scale * gain_ref[...].astype(jnp.float32)[None]).astype(jnp.bfloat16)
            for h in range(HEADS):
                lhs[0, h, at, :] = out[:, h * HEAD : (h + 1) * HEAD]

        lax.fori_loop(0, 4, rows, None)

    def kv_project(which):
        if which == 0:
            for q in range(4):
                pltpu.make_async_copy(own_kv(q), kv_all.at[z, r, q], l_sem.at[0]).start()
            got(kv_all.at[z, r], l_sem.at[0])
            for k in range(4):
                handed(KV, z if k == 0 else source(k))

        def loop(n, _):
            total = acc[which]
            for half in range(2):
                w = kv_all[lax.div(n, 2), lax.rem(n, 2), 2 * half + which]
                total += _dot(lhs[0, 2 * n + half], w, 1, 0)
            acc[which] = total

        acc[which] = jnp.zeros((OWN, HEAD), jnp.float32)
        lax.fori_loop(0, 8, loop, None, unroll=2)
        if which == 0:
            ks[sp] = _turn(acc[0].astype(jnp.bfloat16).astype(jnp.float32), cos_ref[...], sin_ref[...])
        else:
            vts[sp, pl.ds(0, HEAD), :] = acc[1].T.astype(jnp.bfloat16)
            for i in range(8):
                vts[i, pl.ds(HEAD, 16), :] = jnp.ones((16, OWN), jnp.bfloat16)

    def load(t, k):
        b = k % 2
        if k:
            s = source(k)
            handed(t, s)
            pltpu.make_async_copy(w_all.at[t, s], wt.at[b], l_sem.at[b]).start()
        else:
            handed(t, z)
            pltpu.make_async_copy(w_all.at[t, z, other], wt.at[b, other], l_sem.at[b]).start()

            def go(ref, c):
                for q in range(4):
                    pltpu.make_async_copy(columns(ref, q, c), wt.at[b, r, q], l_sem.at[b]).start()

            @pl.when(t < CHUNKS)
            def _():
                go(wq, t)

            @pl.when(t >= CHUNKS)
            def _():
                go(wo, t - CHUNKS)

    def mm(t, k):
        b = k % 2
        got(wt.at[b], l_sem.at[b])
        s = source(k) if k else z
        m = lax.div(t, CHUNKS)

        def one(q, _):
            total = None
            for rr in range(2):
                for half in range(2):
                    d = _dot(lhs[m, 4 * s + 2 * rr + half], wt[b, rr, q, pl.ds(half * 256, 256), :], 1, 0)
                    total = d if total is None else total + d
            acc[q] = total if k == 0 else acc[q] + total

        lax.fori_loop(0, 4, one, None, unroll=2)

    def half(t, k, rr, then=None):
        b = k % 2
        got(wt.at[b, rr], l_sem.at[b])
        s, m = source(k), t // CHUNKS

        def one(q, _):
            total = acc[q]
            for i in range(2):
                total += _dot(lhs[m, 4 * s + 2 * rr + i], wt[b, rr, q, pl.ds(i * 256, 256), :], 1, 0)
            acc[q] = total
            if then is not None:
                then(q)

        lax.fori_loop(0, 4, one, None)

    def put(t, q):
        at = pl.ds(pl.multiple_of((q * CHUNKS + t - CHUNKS) * HEAD, HEAD), HEAD)
        y_ref[:, at] = (xv[:, at].astype(jnp.float32) + acc[q]).astype(jnp.bfloat16)

    def finish(t):
        @pl.when(t < CHUNKS)
        def _():
            def one(q, _):
                v = acc[q].astype(jnp.bfloat16).astype(jnp.float32)
                qs[q * CHUNKS + t] = _turn(v, cos_ref[...], sin_ref[...])

            lax.fori_loop(0, 4, one, None)

        @pl.when(t >= CHUNKS)
        def _():
            lax.fori_loop(0, 4, lambda q, _: put(t, q), None)

    def attend(n, near):
        e = HEAD**-0.5 * LOG2E
        heads = []
        for i in range(GROUP):
            at = n * GROUP + i
            heads.append(lax.rem(at, 4) * CHUNKS + lax.div(at, 4))
        if near:
            for h in heads:
                top_s[h] = jnp.full((1, OWN), NEG, jnp.float32)
                mix_s[h] = jnp.zeros((HEAD + 8, OWN), jnp.float32)

        def block(j, n, masked):
            keys = ks[pl.ds(j, n)].reshape(n * OWN, HEAD)
            scores = [_dot(keys, qs[h], 1, 1) for h in heads]
            weights, keeps = [], []
            for h, s in zip(heads, scores):
                if masked:
                    key = lax.broadcasted_iota(jnp.int32, (OWN, OWN), 0)
                    own = jnp.where(lax.broadcasted_iota(jnp.int32, (OWN, OWN), 1) >= key, s[(n - 1) * OWN :], HIDDEN)
                    s = jnp.concatenate([s[: (n - 1) * OWN], own], axis=0) if n > 1 else own
                old = top_s[h]
                top = jnp.maximum(old, s.max(axis=0, keepdims=True))
                top_s[h] = top
                weights.append(jnp.exp2((s - top) * e).astype(jnp.bfloat16))
                keeps.append(jnp.exp2((old - top) * e))
            values = [vts[j + i, pl.ds(0, HEAD + 8), :] for i in range(n)]
            for h, w, keep in zip(heads, weights, keeps):
                total = mix_s[h] * keep
                for i in range(n):
                    total += _dot(values[i], w[i * OWN : (i + 1) * OWN], 1, 0)
                mix_s[h] = total

        far = jnp.maximum(z - 1, 0)
        if near:
            pl.when(z > 0)(lambda: block(2 * (z - 1), 2, False))
            pl.when(r == 0)(lambda: block(sp, 1, True))
            pl.when(r == 1)(lambda: block(sp - 1, 2, True))
        else:
            lax.fori_loop(0, far, lambda j, _: block(2 * j, 2, False), None)
            for h in heads:
                lhs[1, h] = (mix_s[h, pl.ds(0, HEAD), :] * (1 / mix_s[h, pl.ds(HEAD, 1), :])).T.astype(jnp.bfloat16)

    barrier = pltpu.get_barrier_semaphore()
    for dev in (DEV_IN, DEV_X, DEV_Y, DEV_D):
        pl.semaphore_signal(barrier, inc=1, device_id=dev, device_id_type=MESH)

    @pl.when(inner)
    def _():
        pl.semaphore_signal(barrier, inc=1, device_id=DEV_OUT, device_id_type=MESH)

    if COMPUTE:
        pltpu.make_async_copy(x_hbm, xv, x_sem.at[0]).start()

    @pl.when(inner)
    def _():
        pl.semaphore_wait(barrier, 5)

    @pl.when(outer)
    def _():
        pl.semaphore_wait(barrier, 4)

    LAST = 2 * CHUNKS - 1

    def guarded(t, low, high, fn):
        if isinstance(t, int):
            if low <= t <= high:
                fn()
        else:
            pl.when((t >= low) & (t <= high))(fn)

    def shifted(stage, t, k, by, but=None):
        at = k - 1 + by
        dt, kk = at // 3, at % 3 + 1
        if isinstance(t, int):
            if 0 <= t + dt <= LAST:
                stage(t + dt, kk)
        elif dt == 0 and but and kk in but[1]:
            pl.when(t != but[0])(lambda: stage(t, kk))
        elif dt == 0:
            stage(t, kk)
        else:
            pl.when((t + dt >= 0) & (t + dt <= LAST))(lambda: stage(t + dt, kk))

    def compute(fn, *args):
        if COMPUTE:
            fn(*args)

    send_own_kv()
    send_own(0)
    stage0(KV, 1)
    compute(got, xv, x_sem.at[0])
    stage1(KV, 1)
    compute(norm, 0)
    stage0(0, 1)
    stage1(0, 1)
    stage0(KV, 2)
    stage2(KV, 1)
    stage0(KV, 3)
    stage1(KV, 2)
    compute(norm, 1)
    stage0(0, 2)
    stage1(KV, 3)
    stage3(KV, 1)
    stage2(KV, 2)
    stage0(0, 3)
    stage1(0, 2)
    pl.when(outer)(lambda: send_own(1))
    compute(norm, 2)
    stage2(KV, 3)
    stage3(KV, 2)
    compute(norm, 3)
    compute(tables)

    def whole(t):
        for k in range(1, 4):
            load(t, k)
            mm(t, k - 1)
        load(t + 1, 0)
        mm(t, 3)
        finish(t)

    def _all(fns):
        for fn in fns:
            fn()

    def round_(t, _):
        pl.when(outer & (t < LAST - 1))(lambda: send_own(t + 2))
        pl.when(inner & (t < LAST))(lambda: send_own(t + 1))
        before = t - 1
        early = lambda *fns: compute(guarded, t, 1, CHUNKS, lambda: _all(fns))

        def ticks(k, mid):
            shifted(stage0, t, k, A0)
            shifted(stage1, t, k, 0, (0, (1, 2, 3)))
            mid[0]()
            shifted(stage2, t, k, -A2)
            mid[1]()
            shifted(stage3, t, k, -A3)
            mid[2]()

        def near(i):
            compute(guarded, t, 2, 5, lambda: attend(2 * (t - 2) + i, True))

        def far(i, low=4):
            compute(guarded, t, low, 6, lambda: attend(lax.div(5 * (t - 4), 2) + i, False))

        def nothing():
            pass

        def mid1():
            early(lambda: load(before, 1), lambda: mm(before, 0))
            compute(guarded, t, 7, 7, lambda: whole(5))

        def mid2():
            compute(guarded, t, 2, 2, lambda: kv_handed((0, 1)))
            compute(guarded, t, 4, 4, lambda: (kv_take(3), kv_handed((2, 3))) and None)
            near(0)

        def mid4():
            early(lambda: load(before, 2), lambda: mm(before, 1))

        def mid5():
            guarded(t, 0, 0, lambda: (stage1(0, 3), stage3(KV, 3)) and None)
            near(1)

        def mid6():
            compute(guarded, t, 0, 0, lambda: kv_project(0))
            far(1)
            compute(guarded, t, 7, 7, lambda: whole(6))

        def mid7():
            compute(guarded, t, 1, 1, lambda: pl.when(z < 3)(lambda: kv_take(1)))
            compute(guarded, t, 2, 2, lambda: pl.when(z < 3)(lambda: kv_take(2)))
            compute(guarded, t, 3, 3, lambda: pl.when(z == 3)(lambda: kv_take(2)))
            early(lambda: load(before, 3), lambda: mm(before, 2))
            compute(guarded, t, 6, 6, lambda: load(4, 0))

        def mid8():
            compute(guarded, t, 0, 0, lambda: kv_project(1))
            far(2, 5)

        def mid9():
            early(lambda: mm(before, 3), lambda: finish(before))
            compute(guarded, t, 0, 0, lambda: kv_send(z, True))
            compute(guarded, t, 6, 6, lambda: whole(4))

        early(lambda: load(before, 0))
        compute(guarded, t, 2, 2, lambda: pl.when(z == 3)(lambda: kv_take(1)))
        ticks(1, (mid1, mid2, lambda: far(0)))
        ticks(2, (mid4, mid5, mid6))
        ticks(3, (mid7, mid8, mid9))

    lax.fori_loop(0, 2 * CHUNKS, round_, None)
    assert A3 == A2 + 1
    steps = [(stage, LAST + 1, k, -by) for k in range(1, 4) for stage, by in ((stage2, A2), (stage3, A3))]
    final = steps.index((stage3, LAST + 1, A3, -A3))
    assert final == 3
    compute(load, LAST, 1)
    compute(mm, LAST, 0)
    for step in steps[:final]:
        shifted(*step)
    compute(load, LAST, 2)
    compute(mm, LAST, 1)
    for step in steps[final:]:
        shifted(*step)
    if COMPUTE:
        s = source(3)
        pltpu.make_async_copy(w_all.at[LAST, s, r], wt.at[1, r], l_sem.at[1]).start()
        mm(LAST, 2)
        half(LAST, 3, r)
        handed(LAST, s)
        pltpu.make_async_copy(w_all.at[LAST, s, other], wt.at[1, other], l_sem.at[1]).start()
        half(LAST, 3, other, lambda q: put(LAST, q))
    else:
        for k in range(4):
            handed(KV, source(k) if k else z)
        def hh(t, _):
            for k in range(4):
                handed(t, source(k) if k else z)
        lax.fori_loop(0, 8, hh, None)
    sent(KV)
    lax.fori_loop(0, 2 * CHUNKS, lambda t, _: sent(t), None)
    if COMPUTE:
        kv_sent()


def solution(mesh):
    bf, f32 = jnp.bfloat16, jnp.float32
    any_, vmem = pl.BlockSpec(memory_space=pl.ANY), pl.BlockSpec(memory_space=pltpu.VMEM)
    dma = pltpu.SemaphoreType.DMA

    def step(x, gain, wq, wk, wv, wo):
        half = HEAD // 2
        rate = THETA ** (-np.arange(half, dtype=np.float32) / half)
        rate = jnp.asarray(rate, f32)[None]
        n = KV + 1
        y, _ = pl.pallas_call(
            _kernel,
            in_specs=[any_, vmem, any_, any_, any_, any_, vmem],
            out_specs=[vmem, any_],
            out_shape=[pltpu.VMEM((OWN, D), bf), jax.ShapeDtypeStruct((2 * CHUNKS, 4, 2, 4, OWN, HEAD), bf)],
            scratch_shapes=[
                pltpu.VMEM((OWN, HEAD // 2), f32),
                pltpu.VMEM((OWN, HEAD // 2), f32),
                pltpu.VMEM((4, 2, 4, 256, HEAD), bf),
                pltpu.VMEM((OWN, D), bf),
                pltpu.VMEM((2, HEADS, OWN, HEAD), bf),
                pltpu.VMEM((HEADS, OWN, HEAD), bf),
                pltpu.VMEM((8, OWN, HEAD), bf),
                pltpu.VMEM((8, HEAD + 16, OWN), bf),
                pltpu.VMEM((4, OWN, HEAD), f32),
                pltpu.VMEM((2, 2, 4, OWN, HEAD), bf),
                pltpu.VMEM((HEADS, 1, OWN), f32),
                pltpu.VMEM((HEADS, HEAD + 8, OWN), f32),
                *[dma((n, 4))] * 6,
                *[dma((n,))] * 7,
                *[dma((2, 4))] * 4,
                dma((2,)), dma((1,)),
            ],
            compiler_params=pltpu.CompilerParams(collective_id=0, has_side_effects=True, vmem_limit_bytes=57 * 2**20),
            cost_estimate=pl.CostEstimate(flops=10**11, bytes_accessed=10**8, transcendentals=10**7),
        )(x, gain, wq, wk, wv, wo, rate)
        return y

    tokens, whole = P(("dp", "sp"), None), P("sp", None)
    return jax.shard_map(
        step,
        mesh=mesh,
        in_specs=(tokens, P(None), whole, whole, whole, whole),
        out_specs=tokens,
        check_vma=False,
    )
```

```python
import functools
import itertools

import jax
import jax.numpy as jnp
import numpy as np
from jax import lax
from jax.experimental import pallas as pl
from jax.experimental.pallas import tpu as pltpu
from jax.sharding import PartitionSpec as P

MESH = pl.DeviceIdType.MESH
HEAD = 256
HEADS = 16
THETA = 10000
NEG = -1e30
HIDDEN = 2 * NEG
LOG2E = 1.4426950408889634
OWN = 512
D = 4096
CHUNKS = 4
KV = 2 * CHUNKS
GROUP = 2
COMPUTE = True
BOTH = 80
FIRST = 5
A0, A2, A3 = 3, 1, 2


def _dot(a, b, ca, cb):
    return lax.dot_general(a, b, (((ca,), (cb,)), ((), ())), preferred_element_type=jnp.float32)


def _turn(t, cos, sin):
    a, b = t[:, : HEAD // 2], t[:, HEAD // 2 :]
    return jnp.concatenate([a * cos - b * sin, b * cos + a * sin], axis=1).astype(jnp.bfloat16)


def _kernel(x_hbm, gain_hbm, wq, wk, wv, wo, rate_hbm, y_ref, w_all,
            gain_ref, rate_ref, cos_ref, sin_ref,
            kv_all, xv, lhs, qs, ks, vts, acc, wt, top_s, mix_s,
            recv_z, recv_x, recv_y, recv_xh, recv_yh, recv_d,
            s_up, s_dn, s_x, s_y, s_xh, s_yh, s_d,
            r_kv, r_kvd, s_kv, s_kvd, l_sem, x_sem):
    p, sp = lax.axis_index("dp"), lax.axis_index("sp")
    z, r = lax.div(sp, 2), lax.rem(sp, 2)
    other = 1 - r
    px, py, pd = lax.rem(p + 2, 4), p + 1 - 2 * lax.rem(p, 2), 3 - p
    hi = lax.div(z, 2)
    u = z + hi * (3 - 2 * z)
    step = 2 * (1 - 2 * hi)
    DEV_IN, DEV_OUT = (p, sp + step), (p, sp - step)
    DEV_X, DEV_Y, DEV_D = (px, sp), (py, sp), (p, sp + 1 - 2 * r)
    inner, outer = u == 1, u == 0

    def source(k):
        su = k - u if k == 1 else k
        return su + hi * (3 - 2 * su)

    def send(src, dst, ssem, rsem, dev):
        pltpu.make_async_remote_copy(src_ref=src, dst_ref=dst, send_sem=ssem, recv_sem=rsem, device_id=dev, device_id_type=MESH).start()

    def got(ref, sem):
        pltpu.make_async_copy(ref, ref, sem).wait()

    def piece(t, s, rr, q, low=0, high=None):
        ref, rows = (kv_all.at[s, rr, q], 256) if isinstance(t, int) and t == KV else (w_all.at[t, s, rr, q], OWN)
        high = rows if high is None else high
        return ref if high - low == rows else ref.at[pl.ds(low, high - low)]

    def rows_of(t):
        return 256 if isinstance(t, int) and t == KV else OWN

    def by_kind(fn):
        def call(t, *args):
            if isinstance(t, int):
                fn(t, *args, BOTH if FIRST <= t < KV else 0)
            else:
                pl.when(t < FIRST)(lambda: fn(t, *args, 0))
                pl.when(t >= FIRST)(lambda: fn(t, *args, BOTH))

        return call

    def several(t, n, rows):
        ref = kv_all.at[0, 0] if isinstance(t, int) and t == KV else w_all.at[t, 0, 0]
        return ref.at[pl.ds(0, n), pl.ds(0, rows)] if rows <= OWN else ref.at[pl.ds(0, 4), pl.ds(0, n * rows // 4)]

    def own_kv(q):
        return (wk, wv)[q % 2].at[pl.ds((q // 2) * 256, 256)]

    def columns(ref, q, c):
        return ref.at[:, pl.ds(pl.multiple_of((q * CHUNKS + c) * HEAD, HEAD), HEAD)]

    def send_z(t, s, parts, sem, dev):
        for src, dst in parts:
            send(src, dst, sem.at[t], recv_z.at[t, s], dev)

    def send_own_z(t, parts):
        send_z(t, z, parts, s_up, DEV_IN)
        pl.when(inner)(lambda: send_z(t, z, parts, s_dn, DEV_OUT))

    def send_own_kv():
        for odd in range(2):
            @pl.when(lax.rem(p, 2) == odd)
            def _():
                src = (wk, wv)[odd].at[pl.ds(pl.multiple_of(lax.div(p, 2) * 256, 256), 256)]
                send_own_z(KV, [(src, piece(KV, z, r, p))])
        for q in range(4):
            send(own_kv(q), piece(KV, z, r, q), s_d.at[KV], recv_d.at[KV, z], DEV_D)

    def send_own(t):
        def go(ref, c, b):
            parts = [(columns(ref, p, c), piece(t, z, r, p))]
            if b:
                for low in (0, OWN - b):
                    parts.append((columns(ref, pd, c).at[pl.ds(low, b)], piece(t, z, r, pd, low, low + b)))
            send_own_z(t, parts)
            for q in range(4):
                send(columns(ref, q, c), piece(t, z, r, q), s_d.at[t], recv_d.at[t, z], DEV_D)

        @pl.when(t < CHUNKS)
        def _():
            go(wq, t, 0)

        pl.when((t >= CHUNKS) & (t < FIRST))(lambda: go(wo, t - CHUNKS, 0))
        pl.when(t >= FIRST)(lambda: go(wo, t - CHUNKS, BOTH))

    def hand(t, s, *part):
        send(piece(t, s, r, *part), piece(t, s, r, *part), s_d.at[t], recv_d.at[t, s], DEV_D)

    def along_z(t, b):
        n = rows_of(t)
        return [(p, 0, n)] + ([(pd, 0, b), (pd, n - b, n)] if b else [])

    @by_kind
    def stage0(t, k, b):
        s = source(k)
        parts = [(piece(t, s, r, *part),) * 2 for part in along_z(t, b)]

        @pl.when(inner)
        def _():
            got(several(t, 1, rows_of(t) + 2 * b), recv_z.at[t, s])
            send_z(t, s, parts, *((s_up, DEV_IN) if k == 1 else (s_dn, DEV_OUT)))

    @by_kind
    def stage1(t, k, b):
        s, n = source(k), rows_of(t)
        pl.when(outer)(lambda: got(several(t, 1, n + 2 * b), recv_z.at[t, s]))
        for parts, ssem, rsem, dev in (
            ([(p, 0, n - b), (pd, 0, b)], s_x, recv_x, DEV_X),
            ([(p, b, n), (pd, n - b, n)], s_y, recv_y, DEV_Y),
        ):
            for part in parts if b else parts[:1]:
                send(piece(t, s, r, *part), piece(t, s, r, *part), ssem.at[t], rsem.at[t, s], dev)
        for part in along_z(t, b):
            hand(t, s, *part)

    @by_kind
    def stage2(t, k, b):
        s, n = source(k), rows_of(t)
        for first, second, rsem, part, ssem, rsem2, dev in (
            ((px, 0, n - b), (py, 0, b), recv_x, (px, b, n // 2), s_yh, recv_yh, DEV_Y),
            ((py, b, n), (px, n - b, n), recv_y, (py, n // 2, n - b), s_xh, recv_xh, DEV_X),
        ):
            got(several(t, 1, n), rsem.at[t, s])
            send(piece(t, s, r, *part), piece(t, s, r, *part), ssem.at[t], rsem2.at[t, s], dev)
            hand(t, s, *first)
            if b:
                hand(t, s, *second)

    @by_kind
    def stage3(t, k, b):
        s, n = source(k), rows_of(t)
        for part, rsem in (((pd, b, n // 2), recv_yh), ((pd, n // 2, n - b), recv_xh)):
            got(piece(t, s, r, *part), rsem.at[t, s])
            hand(t, s, *part)

    def handed(t, s):
        ref = kv_all if isinstance(t, int) and t == KV else w_all.at[t]
        got(ref.at[s, other], recv_d.at[t, s])

    @by_kind
    def sent(t, b):
        n = rows_of(t)
        pl.when(outer)(lambda: got(several(t, 1, n + 2 * b), s_up.at[t]))

        @pl.when(inner)
        def _():
            got(several(t, 2, n + 2 * b), s_up.at[t])
            got(several(t, 3, n + 2 * b), s_dn.at[t])

        for sem, rows in ((s_x, n), (s_y, n), (s_xh, n // 2 - b), (s_yh, n // 2 - b)):
            got(several(t, 3, rows), sem.at[t])
        ref = kv_all if isinstance(t, int) and t == KV else w_all.at[t]
        got(ref.at[pl.ds(0, 2)], s_d.at[t])

    def kv_send(s, up):
        i = 2 * s + r
        k_ref, v_ref = ks.at[i], vts.at[i, pl.ds(0, HEAD)]
        send(k_ref, k_ref, s_kvd.at[0, s], r_kvd.at[0, s], DEV_D)
        send(v_ref, v_ref, s_kvd.at[1, s], r_kvd.at[1, s], DEV_D)
        if up:
            @pl.when(z < 3)
            def _():
                send(k_ref, k_ref, s_kv.at[0, s], r_kv.at[0, s], (p, sp + 2))
                send(v_ref, v_ref, s_kv.at[1, s], r_kv.at[1, s], (p, sp + 2))

    def kv_take(j):
        @pl.when(z >= j)
        def _():
            s = z - j
            got(ks.at[2 * s + r], r_kv.at[0, s])
            got(vts.at[2 * s + r, pl.ds(0, HEAD)], r_kv.at[1, s])
            kv_send(s, True)

    def kv_handed(which):
        for j in which:
            @pl.when(z >= j)
            def _():
                s = z - j
                got(ks.at[2 * s + other], r_kvd.at[0, s])
                got(vts.at[2 * s + other, pl.ds(0, HEAD)], r_kvd.at[1, s])

    def kv_sent():
        for j in range(4):
            @pl.when(z >= j)
            def _():
                s = z - j
                for i in range(2):
                    got(ks.at[0], s_kvd.at[i, s])

                    @pl.when(z < 3)
                    def _():
                        got(ks.at[0], s_kv.at[i, s])

    def tables():
        place = lax.broadcasted_iota(jnp.int32, (OWN, HEAD // 2), 0) + sp * OWN
        angle = place.astype(jnp.float32) * rate_ref[...]
        cos_ref[...] = jnp.cos(angle)
        sin_ref[...] = jnp.sin(angle)

    def norm(i):
        def rows(n, _):
            at = pl.ds(pl.multiple_of(i * 128 + n * 32, 32), 32)
            wide = xv[at, :].astype(jnp.float32)
            scale = lax.rsqrt(jnp.mean(wide * wide, axis=-1, keepdims=True) + 1e-6)
            out = (wide * scale * gain_ref[...].astype(jnp.float32)[None]).astype(jnp.bfloat16)
            for h in range(HEADS):
                lhs[0, h, at, :] = out[:, h * HEAD : (h + 1) * HEAD]

        lax.fori_loop(0, 4, rows, None)

    def kv_project(which):
        if which == 0:
            for q in range(4):
                pltpu.make_async_copy(own_kv(q), kv_all.at[z, r, q], l_sem.at[0]).start()
            got(kv_all.at[z, r], l_sem.at[0])
            for k in range(4):
                handed(KV, z if k == 0 else source(k))

        def loop(n, _):
            total = acc[which]
            for half in range(2):
                w = kv_all[lax.div(n, 2), lax.rem(n, 2), 2 * half + which]
                total += _dot(lhs[0, 2 * n + half], w, 1, 0)
            acc[which] = total

        acc[which] = jnp.zeros((OWN, HEAD), jnp.float32)
        lax.fori_loop(0, 8, loop, None, unroll=2)
        if which == 0:
            ks[sp] = _turn(acc[0].astype(jnp.bfloat16).astype(jnp.float32), cos_ref[...], sin_ref[...])
        else:
            vts[sp, pl.ds(0, HEAD), :] = acc[1].T.astype(jnp.bfloat16)
            for i in range(8):
                vts[i, pl.ds(HEAD, 16), :] = jnp.ones((16, OWN), jnp.bfloat16)

    def load(t, k):
        b = k % 2
        if k:
            s = source(k)
            handed(t, s)
            pltpu.make_async_copy(w_all.at[t, s], wt.at[b], l_sem.at[b]).start()
        else:
            handed(t, z)
            pltpu.make_async_copy(w_all.at[t, z, other], wt.at[b, other], l_sem.at[b]).start()

            def go(ref, c):
                for q in range(4):
                    pltpu.make_async_copy(columns(ref, q, c), wt.at[b, r, q], l_sem.at[b]).start()

            @pl.when(t < CHUNKS)
            def _():
                go(wq, t)

            @pl.when(t >= CHUNKS)
            def _():
                go(wo, t - CHUNKS)

    def mm(t, k):
        b = k % 2
        got(wt.at[b], l_sem.at[b])
        s = source(k) if k else z
        m = lax.div(t, CHUNKS)

        def one(q, _):
            total = None
            for rr in range(2):
                for half in range(2):
                    d = _dot(lhs[m, 4 * s + 2 * rr + half], wt[b, rr, q, pl.ds(half * 256, 256), :], 1, 0)
                    total = d if total is None else total + d
            acc[q] = total if k == 0 else acc[q] + total

        lax.fori_loop(0, 4, one, None, unroll=2)

    def half(t, k, rr, then=None):
        b = k % 2
        got(wt.at[b, rr], l_sem.at[b])
        s, m = source(k), t // CHUNKS

        def one(q, _):
            total = acc[q]
            for i in range(2):
                total += _dot(lhs[m, 4 * s + 2 * rr + i], wt[b, rr, q, pl.ds(i * 256, 256), :], 1, 0)
            acc[q] = total
            if then is not None:
                then(q)

        lax.fori_loop(0, 4, one, None, unroll=4)

    def put(t, q):
        at = pl.ds(pl.multiple_of((q * CHUNKS + t - CHUNKS) * HEAD, HEAD), HEAD)
        y_ref[:, at] = (xv[:, at].astype(jnp.float32) + acc[q]).astype(jnp.bfloat16)

    def finish(t):
        @pl.when(t < CHUNKS)
        def _():
            def one(q, _):
                v = acc[q].astype(jnp.bfloat16).astype(jnp.float32)
                qs[q * CHUNKS + t] = _turn(v, cos_ref[...], sin_ref[...])

            lax.fori_loop(0, 4, one, None)

        @pl.when(t >= CHUNKS)
        def _():
            lax.fori_loop(0, 4, lambda q, _: put(t, q), None)

    def attend(n, near):
        e = HEAD**-0.5 * LOG2E
        heads = []
        for i in range(GROUP):
            at = n * GROUP + i
            heads.append(lax.rem(at, 4) * CHUNKS + lax.div(at, 4))
        if near:
            for h in heads:
                top_s[h] = jnp.full((1, OWN), NEG, jnp.float32)
                mix_s[h] = jnp.zeros((HEAD + 8, OWN), jnp.float32)

        def block(j, n, masked):
            keys = ks[pl.ds(j, n)].reshape(n * OWN, HEAD)
            scores = [_dot(keys, qs[h], 1, 1) for h in heads]
            weights, keeps = [], []
            for h, s in zip(heads, scores):
                if masked:
                    key = lax.broadcasted_iota(jnp.int32, (OWN, OWN), 0)
                    own = jnp.where(lax.broadcasted_iota(jnp.int32, (OWN, OWN), 1) >= key, s[(n - 1) * OWN :], HIDDEN)
                    s = jnp.concatenate([s[: (n - 1) * OWN], own], axis=0) if n > 1 else own
                old = top_s[h]
                top = jnp.maximum(old, s.max(axis=0, keepdims=True))
                top_s[h] = top
                weights.append(jnp.exp2((s - top) * e).astype(jnp.bfloat16))
                keeps.append(jnp.exp2((old - top) * e))
            values = [vts[j + i, pl.ds(0, HEAD + 8), :] for i in range(n)]
            for h, w, keep in zip(heads, weights, keeps):
                total = mix_s[h] * keep
                for i in range(n):
                    total += _dot(values[i], w[i * OWN : (i + 1) * OWN], 1, 0)
                mix_s[h] = total

        far = jnp.maximum(z - 1, 0)
        if near:
            pl.when(z > 0)(lambda: block(2 * (z - 1), 2, False))
            pl.when(r == 0)(lambda: block(sp, 1, True))
            pl.when(r == 1)(lambda: block(sp - 1, 2, True))
        else:
            lax.fori_loop(0, far, lambda j, _: block(2 * j, 2, False), None)
            for h in heads:
                lhs[1, h] = (mix_s[h, pl.ds(0, HEAD), :] * (1 / mix_s[h, pl.ds(HEAD, 1), :])).T.astype(jnp.bfloat16)

    barrier = pltpu.get_barrier_semaphore()
    for dev in (DEV_IN, DEV_X, DEV_Y, DEV_D):
        pl.semaphore_signal(barrier, inc=1, device_id=dev, device_id_type=MESH)

    @pl.when(inner)
    def _():
        pl.semaphore_signal(barrier, inc=1, device_id=DEV_OUT, device_id_type=MESH)

    @pl.when(inner)
    def _():
        pl.semaphore_wait(barrier, 5)

    @pl.when(outer)
    def _():
        pl.semaphore_wait(barrier, 4)

    LAST = 2 * CHUNKS - 1

    def guarded(t, low, high, fn):
        if isinstance(t, int):
            if low <= t <= high:
                fn()
        else:
            pl.when((t >= low) & (t <= high))(fn)

    def shifted(stage, t, k, by, but=None):
        at = k - 1 + by
        dt, kk = at // 3, at % 3 + 1
        if isinstance(t, int):
            if 0 <= t + dt <= LAST:
                stage(t + dt, kk)
        elif dt == 0 and but and kk in but[1]:
            pl.when(t != but[0])(lambda: stage(t, kk))
        elif dt == 0:
            stage(t, kk)
        else:
            pl.when((t + dt >= 0) & (t + dt <= LAST))(lambda: stage(t + dt, kk))

    def compute(fn, *args):
        if COMPUTE:
            fn(*args)

    send_own_kv()
    if COMPUTE:
        pltpu.make_async_copy(x_hbm, xv, x_sem.at[0]).start()
        pltpu.make_async_copy(gain_hbm, gain_ref, x_sem.at[1]).start()
        pltpu.make_async_copy(rate_hbm, rate_ref, x_sem.at[2]).start()
    send_own(0)
    stage0(KV, 1)
    stage1(KV, 1)
    compute(got, xv, x_sem.at[0])
    compute(got, gain_ref, x_sem.at[1])
    compute(got, rate_ref, x_sem.at[2])
    compute(norm, 0)
    stage0(0, 1)
    stage1(0, 1)
    stage0(KV, 2)
    stage2(KV, 1)
    stage0(KV, 3)
    stage1(KV, 2)
    compute(norm, 1)
    stage0(0, 2)
    stage1(KV, 3)
    stage3(KV, 1)
    stage2(KV, 2)
    stage0(0, 3)
    stage1(0, 2)
    send_own(1)
    compute(norm, 2)
    stage2(KV, 3)
    stage3(KV, 2)
    compute(norm, 3)
    compute(tables)

    def whole(t):
        for k in range(1, 4):
            load(t, k)
            mm(t, k - 1)
        load(t + 1, 0)
        mm(t, 3)
        finish(t)

    def _all(fns):
        for fn in fns:
            fn()

    def round_(t, _):
        pl.when(outer & (t < LAST - 1))(lambda: send_own(t + 2))
        before = t - 1
        early = lambda *fns: compute(guarded, t, 1, CHUNKS, lambda: _all(fns))

        def ticks(k, mid):
            shifted(stage0, t, k, A0)
            shifted(stage1, t, k, 0, (0, (1, 2, 3)))
            mid[0]()
            shifted(stage2, t, k, -A2)
            mid[1]()
            shifted(stage3, t, k, -A3)
            mid[2]()

        def near(i):
            compute(guarded, t, 2, 5, lambda: attend(2 * (t - 2) + i, True))

        def far(i, low=4):
            compute(guarded, t, low, 6, lambda: attend(3 * (t - 4) + i, False))

        def nothing():
            pass

        def mid1():
            early(lambda: load(before, 1), lambda: mm(before, 0))
            compute(guarded, t, 7, 7, lambda: whole(5))

        def mid2():
            compute(guarded, t, 2, 2, lambda: kv_handed((0, 1)))
            near(0)

        def mid4():
            compute(guarded, t, 4, 4, lambda: kv_take(3))
            early(lambda: load(before, 2), lambda: mm(before, 1))

        def mid5():
            guarded(t, 0, 0, lambda: (stage1(0, 3), stage3(KV, 3)) and None)
            near(1)
            compute(guarded, t, 4, 4, lambda: kv_handed((2, 3)))

        def mid6():
            compute(guarded, t, 0, 0, lambda: kv_project(0))
            far(0)
            compute(guarded, t, 7, 7, lambda: whole(6))

        def mid7():
            compute(guarded, t, 1, 1, lambda: pl.when(z < 3)(lambda: kv_take(1)))
            compute(guarded, t, 2, 2, lambda: pl.when(z < 3)(lambda: kv_take(2)))
            compute(guarded, t, 3, 3, lambda: pl.when(z == 3)(lambda: kv_take(2)))
            early(lambda: load(before, 3), lambda: mm(before, 2))
            compute(guarded, t, 6, 6, lambda: load(4, 0))

        def mid8():
            compute(guarded, t, 0, 0, lambda: kv_project(1))
            far(1)

        def mid9():
            early(lambda: mm(before, 3), lambda: finish(before))
            compute(guarded, t, 0, 0, lambda: kv_send(z, True))
            compute(guarded, t, 6, 6, lambda: whole(4))

        early(lambda: load(before, 0))
        compute(guarded, t, 2, 2, lambda: pl.when(z == 3)(lambda: kv_take(1)))
        ticks(1, (mid1, mid2, lambda: far(-1, 5)))
        ticks(2, (mid4, mid5, mid6))
        pl.when(inner & (t < LAST - 1))(lambda: send_own(t + 2))
        ticks(3, (mid7, mid8, mid9))

    lax.fori_loop(0, 2 * CHUNKS, round_, None)
    assert A3 == A2 + 1
    steps = [(stage, LAST + 1, k, -by) for k in range(1, 4) for stage, by in ((stage2, A2), (stage3, A3))]
    final = steps.index((stage3, LAST + 1, A3, -A3))
    assert final == 3
    compute(load, LAST, 1)
    compute(mm, LAST, 0)
    for step in steps[:final]:
        shifted(*step)
    compute(load, LAST, 2)
    compute(mm, LAST, 1)
    for step in steps[final:]:
        shifted(*step)
    if COMPUTE:
        s = source(3)
        pltpu.make_async_copy(w_all.at[LAST, s, r], wt.at[1, r], l_sem.at[1]).start()
        mm(LAST, 2)
        half(LAST, 3, r)
        handed(LAST, s)
        pltpu.make_async_copy(w_all.at[LAST, s, other], wt.at[1, other], l_sem.at[1]).start()
        half(LAST, 3, other, lambda q: put(LAST, q))
    else:
        for k in range(4):
            handed(KV, source(k) if k else z)
        def hh(t, _):
            for k in range(4):
                handed(t, source(k) if k else z)
        lax.fori_loop(0, 8, hh, None)
    sent(KV)
    lax.fori_loop(0, 2 * CHUNKS, lambda t, _: sent(t), None)
    if COMPUTE:
        kv_sent()


def solution(mesh):
    bf, f32 = jnp.bfloat16, jnp.float32
    any_, vmem = pl.BlockSpec(memory_space=pl.ANY), pl.BlockSpec(memory_space=pltpu.VMEM)
    dma = pltpu.SemaphoreType.DMA

    def step(x, gain, wq, wk, wv, wo):
        half = HEAD // 2
        rate = THETA ** (-np.arange(half, dtype=np.float32) / half)
        rate = jnp.asarray(rate, f32)[None]
        n = KV + 1
        y, _ = pl.pallas_call(
            _kernel,
            in_specs=[any_] * 7,
            out_specs=[vmem, any_],
            out_shape=[pltpu.VMEM((OWN, D), bf), jax.ShapeDtypeStruct((2 * CHUNKS, 4, 2, 4, OWN, HEAD), bf)],
            scratch_shapes=[
                pltpu.VMEM((D,), bf),
                pltpu.VMEM((1, HEAD // 2), f32),
                pltpu.VMEM((OWN, HEAD // 2), f32),
                pltpu.VMEM((OWN, HEAD // 2), f32),
                pltpu.VMEM((4, 2, 4, 256, HEAD), bf),
                pltpu.VMEM((OWN, D), bf),
                pltpu.VMEM((2, HEADS, OWN, HEAD), bf),
                pltpu.VMEM((HEADS, OWN, HEAD), bf),
                pltpu.VMEM((8, OWN, HEAD), bf),
                pltpu.VMEM((8, HEAD + 16, OWN), bf),
                pltpu.VMEM((4, OWN, HEAD), f32),
                pltpu.VMEM((2, 2, 4, OWN, HEAD), bf),
                pltpu.VMEM((HEADS, 1, OWN), f32),
                pltpu.VMEM((HEADS, HEAD + 8, OWN), f32),
                *[dma((n, 4))] * 6,
                *[dma((n,))] * 7,
                *[dma((2, 4))] * 4,
                dma((2,)), dma((3,)),
            ],
            compiler_params=pltpu.CompilerParams(collective_id=0, has_side_effects=True, vmem_limit_bytes=57 * 2**20),
            cost_estimate=pl.CostEstimate(flops=10**11, bytes_accessed=10**8, transcendentals=10**7),
        )(x, gain, wq, wk, wv, wo, rate)
        return y

    tokens, whole = P(("dp", "sp"), None), P("sp", None)
    return jax.shard_map(
        step,
        mesh=mesh,
        in_specs=(tokens, P(None), whole, whole, whole, whole),
        out_specs=tokens,
        check_vma=False,
    )
```

```python
import functools
import itertools

import jax
import jax.numpy as jnp
import numpy as np
from jax import lax
from jax.experimental import pallas as pl
from jax.experimental.pallas import tpu as pltpu
from jax.sharding import PartitionSpec as P

MESH = pl.DeviceIdType.MESH
HEAD = 256
HEADS = 16
THETA = 10000
NEG = -1e30
HIDDEN = 2 * NEG
LOG2E = 1.4426950408889634
OWN = 512
D = 4096
CHUNKS = 4
KV = 2 * CHUNKS
GROUP = 2
BOTH = 80
FIRST = 5
A0, A2, A3 = 3, 1, 2


def _top(n):
    return pl.ds(0, n)


def _times(n, body, unroll=1):
    lax.fori_loop(0, n, body, None, unroll=unroll)


def _dot(a, b, ca=1, cb=0):
    return lax.dot_general(a, b, (((ca,), (cb,)), ((), ())), preferred_element_type=jnp.float32)


def _turn(t, cos, sin):
    a, b = t[:, : HEAD // 2], t[:, HEAD // 2 :]
    return jnp.concatenate([a * cos - b * sin, b * cos + a * sin], axis=1).astype(jnp.bfloat16)


def _kernel(x_hbm, gain_hbm, wq, wk, wv, wo, rate_hbm, y_ref, w_all,
            gain_ref, rate_ref, cos_ref, sin_ref,
            kv_all, xv, lhs, qs, ks, vts, acc, wt, top_s, mix_s,
            recv_z, recv_x, recv_y, recv_xh, recv_yh, recv_d, recv_e,
            s_up, s_dn, s_x, s_y, s_xh, s_yh, s_d,
            r_kv, r_kvd, s_kv, s_kvd, l_sem, x_sem):
    p, sp = lax.axis_index("dp"), lax.axis_index("sp")
    z, r = lax.div(sp, 2), lax.rem(sp, 2)
    other = 1 - r
    px, py, pd = lax.rem(p + 2, 4), p + 1 - 2 * lax.rem(p, 2), 3 - p
    hi = lax.div(z, 2)
    u = z + hi * (3 - 2 * z)
    step = 2 * (1 - 2 * hi)
    DEV_IN, DEV_OUT = (p, sp + step), (p, sp - step)
    DEV_X, DEV_Y, DEV_D = (px, sp), (py, sp), (p, sp + 1 - 2 * r)
    inner, outer = u == 1, u == 0

    def source(k):
        su = k - u if k == 1 else k
        return su + hi * (3 - 2 * su)

    def send(src, dst, ssem, rsem, dev):
        pltpu.make_async_remote_copy(src_ref=src, dst_ref=dst, send_sem=ssem, recv_sem=rsem, device_id=dev, device_id_type=MESH).start()

    def got(ref, sem):
        pltpu.make_async_copy(ref, ref, sem).wait()

    def piece(t, s, rr, q, low=0, high=None):
        ref, rows = (kv_all.at[s, rr, q], 256) if isinstance(t, int) and t == KV else (w_all.at[t, s, rr, q], OWN)
        high = rows if high is None else high
        return ref if high - low == rows else ref.at[pl.ds(low, high - low)]

    def rows_of(t):
        return 256 if isinstance(t, int) and t == KV else OWN

    def turn(t, n):
        return n if isinstance(t, int) and t == KV else t % n if isinstance(t, int) else lax.rem(t, n)

    def group(t, b):
        return 0 if isinstance(t, int) and t == KV else 2 if b else 1

    def by_kind(fn):
        def call(t, *args):
            if isinstance(t, int):
                fn(t, *args, BOTH if FIRST <= t < KV else 0)
            else:
                pl.when(t < FIRST)(lambda: fn(t, *args, 0))
                pl.when(t >= FIRST)(lambda: fn(t, *args, BOTH))

        return call

    def several(t, n, rows):
        ref = kv_all.at[0, 0] if isinstance(t, int) and t == KV else w_all.at[t, 0, 0]
        return ref.at[_top(n), _top(rows)] if rows <= OWN else ref.at[_top(4), _top(n * rows // 4)]

    def own_kv(q):
        return (wk, wv)[q % 2].at[pl.ds((q // 2) * 256, 256)]

    def columns(ref, q, c):
        return ref.at[:, pl.ds(pl.multiple_of((q * CHUNKS + c) * HEAD, HEAD), HEAD)]

    def send_z(t, s, parts, sem, dev, b):
        for src, dst in parts:
            send(src, dst, sem.at[group(t, b)], recv_z.at[turn(t, 4), s], dev)

    def send_own_z(t, parts, b):
        send_z(t, z, parts, s_up, DEV_IN, b)
        pl.when(inner)(lambda: send_z(t, z, parts, s_dn, DEV_OUT, b))

    def send_own_kv():
        for odd in range(2):
            @pl.when(lax.rem(p, 2) == odd)
            def _():
                src = (wk, wv)[odd].at[pl.ds(pl.multiple_of(lax.div(p, 2) * 256, 256), 256)]
                send_own_z(KV, [(src, piece(KV, z, r, p))], 0)
        for q in range(4):
            send(own_kv(q), piece(KV, z, r, q), s_d.at[0], recv_d.at[KV, z], DEV_D)

    def send_own(t):
        def go(ref, c, b):
            parts = [(columns(ref, p, c), piece(t, z, r, p))]
            if b:
                for low in (0, OWN - b):
                    parts.append((columns(ref, pd, c).at[pl.ds(low, b)], piece(t, z, r, pd, low, low + b)))
            send_own_z(t, parts, b)
            for q in range(4):
                send(columns(ref, q, c), piece(t, z, r, q), s_d.at[group(t, b)], recv_d.at[t, z], DEV_D)

        @pl.when(t < CHUNKS)
        def _():
            go(wq, t, 0)

        pl.when((t >= CHUNKS) & (t < FIRST))(lambda: go(wo, t - CHUNKS, 0))
        pl.when(t >= FIRST)(lambda: go(wo, t - CHUNKS, BOTH))

    def hand(t, s, b, *part, rsem=None):
        rsem = recv_d.at[t, s] if rsem is None else rsem
        send(piece(t, s, r, *part), piece(t, s, r, *part), s_d.at[group(t, b)], rsem, DEV_D)

    def along_z(t, b):
        n = rows_of(t)
        return [(p, 0, n)] + ([(pd, 0, b), (pd, n - b, n)] if b else [])

    @by_kind
    def stage0(t, k, b):
        s = source(k)
        parts = [(piece(t, s, r, *part),) * 2 for part in along_z(t, b)]

        @pl.when(inner)
        def _():
            got(several(t, 1, rows_of(t) + 2 * b), recv_z.at[turn(t, 4), s])
            send_z(t, s, parts, *((s_up, DEV_IN) if k == 1 else (s_dn, DEV_OUT)), b)

    @by_kind
    def stage1(t, k, b):
        s, n = source(k), rows_of(t)
        pl.when(outer)(lambda: got(several(t, 1, n + 2 * b), recv_z.at[turn(t, 4), s]))
        for parts, ssem, rsem, dev in (
            ([(p, 0, n - b), (pd, 0, b)], s_x, recv_x, DEV_X),
            ([(p, b, n), (pd, n - b, n)], s_y, recv_y, DEV_Y),
        ):
            for part in parts if b else parts[:1]:
                send(piece(t, s, r, *part), piece(t, s, r, *part), ssem.at[group(t, b)], rsem.at[turn(t, 2), s], dev)
        for part in along_z(t, b):
            hand(t, s, b, *part)

    @by_kind
    def stage2(t, k, b):
        s, n = source(k), rows_of(t)
        for first, second, rsem, part, ssem, rsem2, dev in (
            ((px, 0, n - b), (py, 0, b), recv_x, (px, b, n // 2), s_yh, recv_yh, DEV_Y),
            ((py, b, n), (px, n - b, n), recv_y, (py, n // 2, n - b), s_xh, recv_xh, DEV_X),
        ):
            got(several(t, 1, n), rsem.at[turn(t, 2), s])
            send(piece(t, s, r, *part), piece(t, s, r, *part), ssem.at[group(t, b)], rsem2.at[turn(t, 2), s], dev)
            hand(t, s, b, *first)
            if b:
                hand(t, s, b, *second)

    @by_kind
    def stage3(t, k, b):
        s, n = source(k), rows_of(t)
        for part, rsem in (((pd, b, n // 2), recv_yh), ((pd, n // 2, n - b), recv_xh)):
            got(piece(t, s, r, *part), rsem.at[turn(t, 2), s])
            hand(t, s, b, *part, rsem=recv_e.at[0] if isinstance(t, int) and (t, k) == (KV - 1, 3) else None)

    def handed(t, s):
        ref = kv_all if isinstance(t, int) and t == KV else w_all.at[t]
        got(ref.at[s, other], recv_d.at[t, s])

    def all_sent():
        for i, n, b in ((0, 1, 0), (1, FIRST, 0), (2, KV - FIRST, BOTH)):
            rows = 256 if i == 0 else OWN
            ref = kv_all.at[_top(1)] if i == 0 else w_all.at[_top(n), 0]

            def view(m, length):
                shape = (_top(m), _top(length)) if length <= rows else (_top(4), _top(m * length // 4))
                return ref.at[_top(n), 0, *shape]

            pl.when(outer)(lambda: got(view(1, rows + 2 * b), s_up.at[i]))

            @pl.when(inner)
            def _():
                got(view(2, rows + 2 * b), s_up.at[i])
                got(view(3, rows + 2 * b), s_dn.at[i])

            for sem, length in ((s_x, rows), (s_y, rows), (s_xh, rows // 2 - b), (s_yh, rows // 2 - b)):
                got(view(3, length), sem.at[i])
            got(kv_all.at[_top(2)] if i == 0 else w_all.at[_top(n), _top(2)], s_d.at[i])

    def kv_send(s, up):
        i = 2 * s + r
        k_ref, v_ref = ks.at[i], vts.at[i, _top(HEAD)]
        send(k_ref, k_ref, s_kvd.at[0, s], r_kvd.at[0, s], DEV_D)
        send(v_ref, v_ref, s_kvd.at[1, s], r_kvd.at[1, s], DEV_D)
        if up:
            @pl.when(z < 3)
            def _():
                send(k_ref, k_ref, s_kv.at[0, s], r_kv.at[0, s], (p, sp + 2))
                send(v_ref, v_ref, s_kv.at[1, s], r_kv.at[1, s], (p, sp + 2))

    def kv_take(j):
        @pl.when(z >= j)
        def _():
            s = z - j
            got(ks.at[2 * s + r], r_kv.at[0, s])
            got(vts.at[2 * s + r, _top(HEAD)], r_kv.at[1, s])
            kv_send(s, True)

    def kv_handed(which):
        for j in which:
            @pl.when(z >= j)
            def _():
                s = z - j
                got(ks.at[2 * s + other], r_kvd.at[0, s])
                got(vts.at[2 * s + other, _top(HEAD)], r_kvd.at[1, s])

    def kv_sent():
        for j in range(4):
            @pl.when(z >= j)
            def _():
                s = z - j
                for i in range(2):
                    got(ks.at[0], s_kvd.at[i, s])

                    @pl.when(z < 3)
                    def _():
                        got(ks.at[0], s_kv.at[i, s])

    def tables():
        place = lax.broadcasted_iota(jnp.int32, (OWN, HEAD // 2), 0) + sp * OWN
        angle = place.astype(jnp.float32) * rate_ref[...]
        cos_ref[...] = jnp.cos(angle)
        sin_ref[...] = jnp.sin(angle)

    def norm(i):
        def rows(n, _):
            at = pl.ds(pl.multiple_of(i * 128 + n * 32, 32), 32)
            wide = xv[at, :].astype(jnp.float32)
            scale = lax.rsqrt(jnp.mean(wide * wide, axis=-1, keepdims=True) + 1e-6)
            out = (wide * scale * gain_ref[...].astype(jnp.float32)[None]).astype(jnp.bfloat16)
            for h in range(HEADS):
                lhs[0, h, at, :] = out[:, h * HEAD : (h + 1) * HEAD]

        _times(4, rows)

    def kv_project(which):
        if which == 0:
            for q in range(4):
                pltpu.make_async_copy(own_kv(q), kv_all.at[z, r, q], l_sem.at[0]).start()
            got(kv_all.at[z, r], l_sem.at[0])
            for k in range(4):
                handed(KV, z if k == 0 else source(k))

        def loop(n, _):
            total = acc[which]
            for half in range(2):
                w = kv_all[lax.div(n, 2), lax.rem(n, 2), 2 * half + which]
                total += _dot(lhs[0, 2 * n + half], w)
            acc[which] = total

        acc[which] = jnp.zeros((OWN, HEAD), jnp.float32)
        _times(8, loop, 2)
        if which == 0:
            ks[sp] = _turn(acc[which].astype(jnp.bfloat16).astype(jnp.float32), cos_ref[...], sin_ref[...])
        else:
            vts[sp, _top(HEAD), :] = acc[which].T.astype(jnp.bfloat16)
            for i in range(8):
                vts[i, pl.ds(HEAD, 16), :] = jnp.ones((16, OWN), jnp.bfloat16)

    def load(t, k):
        b = k % 2
        if k:
            s = source(k)
            handed(t, s)
            pltpu.make_async_copy(w_all.at[t, s], wt.at[b], l_sem.at[b]).start()
        else:
            handed(t, z)
            pltpu.make_async_copy(w_all.at[t, z, other], wt.at[b, other], l_sem.at[b]).start()

            def go(ref, c):
                for q in range(4):
                    pltpu.make_async_copy(columns(ref, q, c), wt.at[b, r, q], l_sem.at[b]).start()

            @pl.when(t < CHUNKS)
            def _():
                go(wq, t)

            @pl.when(t >= CHUNKS)
            def _():
                go(wo, t - CHUNKS)

    def mm(t, k):
        b = k % 2
        got(wt.at[b], l_sem.at[b])
        s = source(k) if k else z
        m = lax.div(t, CHUNKS)

        def one(q, _):
            total = None
            for rr in range(2):
                for half in range(2):
                    d = _dot(lhs[m, 4 * s + 2 * rr + half], wt[b, rr, q, pl.ds(half * 256, 256), :])
                    total = d if total is None else total + d
            acc[q] = total if k == 0 else acc[q] + total

        _times(4, one, 4)

    def quarter(t, k, q):
        s, m, totals = source(k), t // CHUNKS, []
        for rows in (_top(OWN // 2), pl.ds(OWN // 2, OWN // 2)):
            total = None
            for rr in range(2):
                for i in range(2):
                    d = _dot(lhs[m, 4 * s + 2 * rr + i, rows, :], wt[k % 2, rr, q, pl.ds(i * 256, 256), :])
                    total = d if total is None else total + d
            totals.append(total)
        acc[q] += jnp.concatenate(totals, axis=0)
        put(t, q)

    def put(t, q):
        at = pl.ds(pl.multiple_of((q * CHUNKS + t - CHUNKS) * HEAD, HEAD), HEAD)
        y_ref[:, at] = (xv[:, at].astype(jnp.float32) + acc[q]).astype(jnp.bfloat16)

    def finish(t):
        @pl.when(t < CHUNKS)
        def _():
            def one(q, _):
                v = acc[q].astype(jnp.bfloat16).astype(jnp.float32)
                qs[q * CHUNKS + t] = _turn(v, cos_ref[...], sin_ref[...])

            _times(4, one)

        @pl.when(t >= CHUNKS)
        def _():
            _times(4, lambda q, _: put(t, q))

    def attend(n, near):
        e = HEAD**-0.5 * LOG2E
        heads = []
        for i in range(GROUP):
            at = n * GROUP + i
            heads.append(lax.rem(at, 4) * CHUNKS + lax.div(at, 4))
        if near:
            for h in heads:
                top_s[h] = jnp.full((1, OWN), NEG, jnp.float32)
                mix_s[h] = jnp.zeros((HEAD + 8, OWN), jnp.float32)

        def block(j, n, masked):
            keys = ks[pl.ds(j, n)].reshape(n * OWN, HEAD)
            scores = [_dot(keys, qs[h], 1, 1) for h in heads]
            weights, keeps = [], []
            for h, s in zip(heads, scores):
                if masked:
                    key = lax.broadcasted_iota(jnp.int32, (OWN, OWN), 0)
                    own = jnp.where(lax.broadcasted_iota(jnp.int32, (OWN, OWN), 1) >= key, s[(n - 1) * OWN :], HIDDEN)
                    s = jnp.concatenate([s[: (n - 1) * OWN], own], axis=0) if n > 1 else own
                old = top_s[h]
                top = jnp.maximum(old, s.max(axis=0, keepdims=True))
                top_s[h] = top
                weights.append(jnp.exp2((s - top) * e).astype(jnp.bfloat16))
                keeps.append(jnp.exp2((old - top) * e))
            values = [vts[j + i, _top(HEAD + 8), :] for i in range(n)]
            for h, w, keep in zip(heads, weights, keeps):
                total = mix_s[h] * keep
                for i in range(n):
                    total += _dot(values[i], w[i * OWN : (i + 1) * OWN])
                mix_s[h] = total

        far = jnp.maximum(z - 1, 0)
        if near:
            pl.when(z > 0)(lambda: block(2 * (z - 1), 2, False))
            pl.when(r == 0)(lambda: block(sp, 1, True))
            pl.when(r == 1)(lambda: block(sp - 1, 2, True))
        else:
            _times(far, lambda j, _: block(2 * j, 2, False))
            for h in heads:
                lhs[1, h] = (mix_s[h, _top(HEAD), :] * (1 / mix_s[h, pl.ds(HEAD, 1), :])).T.astype(jnp.bfloat16)

    barrier = pltpu.get_barrier_semaphore()
    for dev in (DEV_IN, DEV_X, DEV_Y, DEV_D):
        pl.semaphore_signal(barrier, inc=1, device_id=dev, device_id_type=MESH)

    @pl.when(inner)
    def _():
        pl.semaphore_signal(barrier, inc=1, device_id=DEV_OUT, device_id_type=MESH)

    @pl.when(inner)
    def _():
        pl.semaphore_wait(barrier, 5)

    @pl.when(outer)
    def _():
        pl.semaphore_wait(barrier, 4)

    LAST = KV - 1

    def guarded(t, low, high, fn):
        if isinstance(t, int):
            if low <= t <= high:
                fn()
        else:
            pl.when((t >= low) & (t <= high))(fn)

    def in_round(t, n, fn):
        pl.when(t == n)(fn)

    def shifted(stage, t, k, by, but=None):
        at = k - 1 + by
        dt, kk = at // 3, at % 3 + 1
        if isinstance(t, int):
            if 0 <= t + dt <= LAST:
                stage(t + dt, kk)
        elif dt == 0 and but and kk in but[1]:
            pl.when(t != but[0])(lambda: stage(t, kk))
        elif dt == 0:
            stage(t, kk)
        else:
            pl.when((t + dt >= 0) & (t + dt <= LAST))(lambda: stage(t + dt, kk))

    send_own_kv()
    pltpu.make_async_copy(x_hbm, xv, x_sem.at[0]).start()
    pltpu.make_async_copy(gain_hbm, gain_ref, x_sem.at[1]).start()
    pltpu.make_async_copy(rate_hbm, rate_ref, x_sem.at[2]).start()
    send_own(0)
    stage0(KV, 1)
    stage1(KV, 1)
    got(xv, x_sem.at[0])
    got(gain_ref, x_sem.at[1])
    got(rate_ref, x_sem.at[2])
    norm(0)
    stage0(0, 1)
    stage1(0, 1)
    stage0(KV, 2)
    stage2(KV, 1)
    stage0(KV, 3)
    stage1(KV, 2)
    norm(1)
    stage0(0, 2)
    stage1(KV, 3)
    stage3(KV, 1)
    stage2(KV, 2)
    stage0(0, 3)
    stage1(0, 2)
    send_own(1)
    norm(2)
    stage2(KV, 3)
    stage3(KV, 2)
    norm(3)
    tables()

    def whole(t):
        for k in range(1, 4):
            load(t, k)
            mm(t, k - 1)
        load(t + 1, 0)
        mm(t, 3)
        finish(t)

    def _all(fns):
        for fn in fns:
            fn()

    def round_(t, _):
        pl.when(outer & (t < LAST - 1))(lambda: send_own(t + 2))
        before = t - 1
        early = lambda *fns: guarded(t, 1, CHUNKS, lambda: _all(fns))

        def ticks(k, mid):
            shifted(stage0, t, k, A0)
            shifted(stage1, t, k, 0, (0, (1, 2, 3)))
            mid[0]()
            shifted(stage2, t, k, -A2)
            mid[1]()
            shifted(stage3, t, k, -A3)
            mid[2]()

        def near(i):
            guarded(t, 2, 5, lambda: attend(2 * (t - 2) + i, True))

        def far(i, low=4):
            guarded(t, low, 6, lambda: attend(3 * (t - 4) + i, False))

        def nothing():
            pass

        def mid1():
            early(lambda: load(before, 1), lambda: mm(before, 0))
            in_round(t, 7, lambda: whole(5))

        def mid2():
            in_round(t, 2, lambda: kv_handed((0, 1)))
            near(0)

        def mid4():
            in_round(t, 4, lambda: kv_take(3))
            early(lambda: load(before, 2), lambda: mm(before, 1))

        def mid5():
            in_round(t, 0, lambda: _all((lambda: stage1(0, 3), lambda: stage3(KV, 3))))
            near(1)
            in_round(t, 4, lambda: kv_handed((2, 3)))

        def mid6():
            in_round(t, 0, lambda: kv_project(0))
            far(0)
            in_round(t, 7, lambda: whole(6))

        def mid7():
            in_round(t, 1, lambda: pl.when(z < 3)(lambda: kv_take(1)))
            in_round(t, 2, lambda: pl.when(z < 3)(lambda: kv_take(2)))
            in_round(t, 3, lambda: pl.when(z == 3)(lambda: kv_take(2)))
            early(lambda: load(before, 3), lambda: mm(before, 2))
            in_round(t, 6, lambda: load(4, 0))

        def mid8():
            in_round(t, 0, lambda: kv_project(1))
            far(1)

        def mid9():
            early(lambda: mm(before, 3), lambda: finish(before))
            in_round(t, 0, lambda: kv_send(z, True))
            in_round(t, 6, lambda: whole(4))

        early(lambda: load(before, 0))
        in_round(t, 2, lambda: pl.when(z == 3)(lambda: kv_take(1)))
        ticks(1, (mid1, mid2, lambda: far(-1, 5)))
        ticks(2, (mid4, mid5, mid6))
        pl.when(inner & (t < LAST - 1))(lambda: send_own(t + 2))
        ticks(3, (mid7, mid8, mid9))

    _times(KV, round_)
    assert A3 == A2 + 1
    steps = [(stage, LAST + 1, k, -by) for k in range(1, 4) for stage, by in ((stage2, A2), (stage3, A3))]
    final = steps.index((stage3, LAST + 1, A3, -A3))
    assert final == 3
    load(LAST, 1)
    mm(LAST, 0)
    for step in steps[:final]:
        shifted(*step)
    mm(LAST, 1)
    load(LAST, 2)
    for step in steps[final:]:
        shifted(*step)
    s = source(3)
    pltpu.make_async_copy(w_all.at[LAST, s, r], wt.at[1, r], l_sem.at[1]).start()
    got(w_all.at[LAST, s, other, _top(4), _top(OWN - (OWN - 2 * BOTH) // 4)], recv_d.at[LAST, s])
    for q in (p, px, py):
        pltpu.make_async_copy(w_all.at[LAST, s, other, q], wt.at[1, other, q], x_sem.at[1]).start()
    mm(LAST, 2)
    got(wt.at[1, r], l_sem.at[1])
    got(wt.at[1, other, _top(3)], x_sem.at[1])
    quarter(LAST, 3, p)
    quarter(LAST, 3, px)
    got(w_all.at[LAST, s, other, pd, pl.ds(BOTH, OWN - 2 * BOTH)], recv_e.at[0])
    last = pltpu.make_async_copy(w_all.at[LAST, s, other, pd], wt.at[1, other, pd], l_sem.at[1])
    last.start()
    quarter(LAST, 3, py)
    last.wait()
    quarter(LAST, 3, pd)
    all_sent()
    kv_sent()


def solution(mesh):
    bf, f32 = jnp.bfloat16, jnp.float32
    any_, vmem = pl.BlockSpec(memory_space=pl.ANY), pl.BlockSpec(memory_space=pltpu.VMEM)
    dma = pltpu.SemaphoreType.DMA

    def step(x, gain, wq, wk, wv, wo):
        half = HEAD // 2
        rate = THETA ** (-np.arange(half, dtype=np.float32) / half)
        rate = jnp.asarray(rate, f32)[None]
        y, _ = pl.pallas_call(
            _kernel,
            in_specs=[any_] * 7,
            out_specs=[vmem, any_],
            out_shape=[pltpu.VMEM((OWN, D), bf), jax.ShapeDtypeStruct((KV, 4, 2, 4, OWN, HEAD), bf)],
            scratch_shapes=[
                pltpu.VMEM((D,), bf),
                pltpu.VMEM((1, HEAD // 2), f32),
                pltpu.VMEM((OWN, HEAD // 2), f32),
                pltpu.VMEM((OWN, HEAD // 2), f32),
                pltpu.VMEM((4, 2, 4, 256, HEAD), bf),
                pltpu.VMEM((OWN, D), bf),
                pltpu.VMEM((2, HEADS, OWN, HEAD), bf),
                pltpu.VMEM((HEADS, OWN, HEAD), bf),
                pltpu.VMEM((8, OWN, HEAD), bf),
                pltpu.VMEM((8, HEAD + 16, OWN), bf),
                pltpu.VMEM((4, OWN, HEAD), f32),
                pltpu.VMEM((2, 2, 4, OWN, HEAD), bf),
                pltpu.VMEM((HEADS, 1, OWN), f32),
                pltpu.VMEM((HEADS, HEAD + 8, OWN), f32),
                dma((5, 4)), *[dma((3, 4))] * 4, dma((KV + 1, 4)), dma((1,)),
                *[dma((3,))] * 7,
                *[dma((2, 4))] * 4,
                dma((2,)), dma((3,)),
            ],
            compiler_params=pltpu.CompilerParams(collective_id=0, has_side_effects=True, vmem_limit_bytes=57 * 2**20),
        )(x, gain, wq, wk, wv, wo, rate)
        return y

    tokens, whole = P(("dp", "sp"), None), P("sp", None)
    return jax.shard_map(
        step,
        mesh=mesh,
        in_specs=(tokens, P(None), whole, whole, whole, whole),
        out_specs=tokens,
        check_vma=False,
    )
```

```python
import functools
import itertools

import jax
import jax.numpy as jnp
import numpy as np
from jax import lax
from jax.experimental import pallas as pl
from jax.experimental.pallas import tpu as pltpu
from jax.sharding import PartitionSpec as P

MESH = pl.DeviceIdType.MESH
HEAD = 256
HEADS = 16
THETA = 10000
NEG = -1e30
HIDDEN = 2 * NEG
LOG2E = 1.4426950408889634
OWN = 512
D = 4096
CHUNKS = 4
KV = 2 * CHUNKS
GROUP = 2
BOTH = 80
FIRST = 5
A0, A2, A3 = 3, 1, 2


def _top(n):
    return pl.ds(0, n)


def _times(n, body, unroll=1):
    lax.fori_loop(0, n, body, None, unroll=unroll)


def _dot(a, b, ca=1, cb=0):
    return lax.dot_general(a, b, (((ca,), (cb,)), ((), ())), preferred_element_type=jnp.float32)


def _turn(t, cos, sin):
    a, b = t[:, : HEAD // 2], t[:, HEAD // 2 :]
    return jnp.concatenate([a * cos - b * sin, b * cos + a * sin], axis=1).astype(jnp.bfloat16)


def _kernel(x_hbm, gain_hbm, wq, wk, wv, wo, rate_hbm, y_ref, w_all,
            gain_ref, rate_ref, cos_ref, sin_ref,
            kv_all, xv, lhs, qs, ks, vts, acc, wt, top_s, mix_s,
            recv_z, recv_x, recv_y, recv_xh, recv_yh, recv_d, recv_e,
            s_up, s_dn, s_x, s_y, s_xh, s_yh, s_d,
            r_kv, r_kvd, s_kv, s_kvd, l_sem, x_sem):
    p, sp = lax.axis_index("dp"), lax.axis_index("sp")
    z, r = lax.div(sp, 2), lax.rem(sp, 2)
    other = 1 - r
    px, py, pd = lax.rem(p + 2, 4), p + 1 - 2 * lax.rem(p, 2), 3 - p
    hi = lax.div(z, 2)
    u = z + hi * (3 - 2 * z)
    step = 2 * (1 - 2 * hi)
    DEV_IN, DEV_OUT = (p, sp + step), (p, sp - step)
    DEV_X, DEV_Y, DEV_D = (px, sp), (py, sp), (p, sp + 1 - 2 * r)
    inner, outer = u == 1, u == 0

    def source(k):
        su = k - u if k == 1 else k
        return su + hi * (3 - 2 * su)

    def send(src, dst, ssem, rsem, dev):
        pltpu.make_async_remote_copy(src_ref=src, dst_ref=dst, send_sem=ssem, recv_sem=rsem, device_id=dev, device_id_type=MESH).start()

    def got(ref, sem):
        pltpu.make_async_copy(ref, ref, sem).wait()

    def piece(t, s, rr, q, low=0, high=None):
        ref, rows = (kv_all.at[s, rr, q], 256) if isinstance(t, int) and t == KV else (w_all.at[t, s, rr, q], OWN)
        high = rows if high is None else high
        return ref if high - low == rows else ref.at[pl.ds(low, high - low)]

    def rows_of(t):
        return 256 if isinstance(t, int) and t == KV else OWN

    def turn(t, n):
        return n if isinstance(t, int) and t == KV else t % n if isinstance(t, int) else lax.rem(t, n)

    def group(t, b):
        return 0 if isinstance(t, int) and t == KV else 2 if b else 1

    def by_kind(fn):
        def call(t, *args):
            if isinstance(t, int):
                fn(t, *args, BOTH if FIRST <= t < KV else 0)
            else:
                pl.when(t < FIRST)(lambda: fn(t, *args, 0))
                pl.when(t >= FIRST)(lambda: fn(t, *args, BOTH))

        return call

    def several(t, n, rows):
        ref = kv_all.at[0, 0] if isinstance(t, int) and t == KV else w_all.at[t, 0, 0]
        return ref.at[_top(n), _top(rows)] if rows <= OWN else ref.at[_top(4), _top(n * rows // 4)]

    def own_kv(q):
        return (wk, wv)[q % 2].at[pl.ds((q // 2) * 256, 256)]

    def columns(ref, q, c):
        return ref.at[:, pl.ds(pl.multiple_of((q * CHUNKS + c) * HEAD, HEAD), HEAD)]

    def send_z(t, s, parts, sem, dev, b):
        for src, dst in parts:
            send(src, dst, sem.at[group(t, b)], recv_z.at[turn(t, 4), s], dev)

    def send_own_z(t, parts, b):
        send_z(t, z, parts, s_up, DEV_IN, b)
        pl.when(inner)(lambda: send_z(t, z, parts, s_dn, DEV_OUT, b))

    def send_own_kv():
        for odd in range(2):
            @pl.when(lax.rem(p, 2) == odd)
            def _():
                src = (wk, wv)[odd].at[pl.ds(pl.multiple_of(lax.div(p, 2) * 256, 256), 256)]
                send_own_z(KV, [(src, piece(KV, z, r, p))], 0)
        for q in range(4):
            send(own_kv(q), piece(KV, z, r, q), s_d.at[0], recv_d.at[turn(KV, 4), z], DEV_D)

    def send_own(t):
        def go(ref, c, b):
            parts = [(columns(ref, p, c), piece(t, z, r, p))]
            if b:
                for low in (0, OWN - b):
                    parts.append((columns(ref, pd, c).at[pl.ds(low, b)], piece(t, z, r, pd, low, low + b)))
            send_own_z(t, parts, b)
            for q in range(4):
                send(columns(ref, q, c), piece(t, z, r, q), s_d.at[group(t, b)], recv_d.at[turn(t, 4), z], DEV_D)

        @pl.when(t < CHUNKS)
        def _():
            go(wq, t, 0)

        pl.when((t >= CHUNKS) & (t < FIRST))(lambda: go(wo, t - CHUNKS, 0))
        pl.when(t >= FIRST)(lambda: go(wo, t - CHUNKS, BOTH))

    def hand(t, s, b, *part, rsem=None):
        rsem = recv_d.at[turn(t, 4), s] if rsem is None else rsem
        send(piece(t, s, r, *part), piece(t, s, r, *part), s_d.at[group(t, b)], rsem, DEV_D)

    def along_z(t, b):
        n = rows_of(t)
        return [(p, 0, n)] + ([(pd, 0, b), (pd, n - b, n)] if b else [])

    @by_kind
    def stage0(t, k, b):
        s = source(k)
        parts = [(piece(t, s, r, *part),) * 2 for part in along_z(t, b)]

        @pl.when(inner)
        def _():
            got(several(t, 1, rows_of(t) + 2 * b), recv_z.at[turn(t, 4), s])
            send_z(t, s, parts, *((s_up, DEV_IN) if k == 1 else (s_dn, DEV_OUT)), b)

    @by_kind
    def stage1(t, k, b):
        s, n = source(k), rows_of(t)
        pl.when(outer)(lambda: got(several(t, 1, n + 2 * b), recv_z.at[turn(t, 4), s]))
        for parts, ssem, rsem, dev in (
            ([(p, 0, n - b), (pd, 0, b)], s_x, recv_x, DEV_X),
            ([(p, b, n), (pd, n - b, n)], s_y, recv_y, DEV_Y),
        ):
            for part in parts if b else parts[:1]:
                send(piece(t, s, r, *part), piece(t, s, r, *part), ssem.at[group(t, b)], rsem.at[turn(t, 2), s], dev)
        for part in along_z(t, b):
            hand(t, s, b, *part)

    @by_kind
    def stage2(t, k, b):
        s, n = source(k), rows_of(t)
        for first, second, rsem, part, ssem, rsem2, dev in (
            ((px, 0, n - b), (py, 0, b), recv_x, (px, b, n // 2), s_yh, recv_yh, DEV_Y),
            ((py, b, n), (px, n - b, n), recv_y, (py, n // 2, n - b), s_xh, recv_xh, DEV_X),
        ):
            got(several(t, 1, n), rsem.at[turn(t, 2), s])
            send(piece(t, s, r, *part), piece(t, s, r, *part), ssem.at[group(t, b)], rsem2.at[turn(t, 2), s], dev)
            hand(t, s, b, *first)
            if b:
                hand(t, s, b, *second)

    @by_kind
    def stage3(t, k, b):
        s, n = source(k), rows_of(t)
        for part, rsem in (((pd, b, n // 2), recv_yh), ((pd, n // 2, n - b), recv_xh)):
            got(piece(t, s, r, *part), rsem.at[turn(t, 2), s])
            hand(t, s, b, *part, rsem=recv_e.at[0] if isinstance(t, int) and (t, k) == (KV - 1, 3) else None)

    def handed(t, s):
        ref = kv_all if isinstance(t, int) and t == KV else w_all.at[t]
        got(ref.at[s, other], recv_d.at[turn(t, 4), s])

    def all_sent():
        for i, n, b in ((0, 1, 0), (1, FIRST, 0), (2, KV - FIRST, BOTH)):
            rows = 256 if i == 0 else OWN
            ref = kv_all.at[_top(1)] if i == 0 else w_all.at[_top(n), 0]

            def view(m, length):
                shape = (_top(m), _top(length)) if length <= rows else (_top(4), _top(m * length // 4))
                return ref.at[_top(n), 0, *shape]

            pl.when(outer)(lambda: got(view(1, rows + 2 * b), s_up.at[i]))

            @pl.when(inner)
            def _():
                got(view(2, rows + 2 * b), s_up.at[i])
                got(view(3, rows + 2 * b), s_dn.at[i])

            for sem, length in ((s_x, rows), (s_y, rows), (s_xh, rows // 2 - b), (s_yh, rows // 2 - b)):
                got(view(3, length), sem.at[i])
            got(kv_all.at[_top(2)] if i == 0 else w_all.at[_top(n), _top(2)], s_d.at[i])

    def kv_send(s, up):
        i = 2 * s + r
        k_ref, v_ref = ks.at[i], vts.at[i, _top(HEAD)]
        send(k_ref, k_ref, s_kvd.at[s], r_kvd.at[s], DEV_D)
        send(v_ref, v_ref, s_kvd.at[s], r_kvd.at[s], DEV_D)
        if up:
            @pl.when(z < 3)
            def _():
                send(k_ref, k_ref, s_kv.at[s], r_kv.at[s], (p, sp + 2))
                send(v_ref, v_ref, s_kv.at[s], r_kv.at[s], (p, sp + 2))

    def kv_take(j):
        @pl.when(z >= j)
        def _():
            s = z - j
            got(ks.at[_top(2)], r_kv.at[s])
            kv_send(s, True)

    def kv_handed(which):
        for j in which:
            @pl.when(z >= j)
            def _():
                s = z - j
                got(ks.at[_top(2)], r_kvd.at[s])

    def kv_sent():
        for j in range(4):
            @pl.when(z >= j)
            def _():
                s = z - j
                got(ks.at[_top(2)], s_kvd.at[s])
                pl.when(z < 3)(lambda: got(ks.at[_top(2)], s_kv.at[s]))

    def tables():
        place = lax.broadcasted_iota(jnp.int32, (OWN, HEAD // 2), 0) + sp * OWN
        angle = place.astype(jnp.float32) * rate_ref[...]
        cos_ref[...] = jnp.cos(angle)
        sin_ref[...] = jnp.sin(angle)

    def norm(i):
        def rows(n, _):
            at = pl.ds(pl.multiple_of(i * 128 + n * 32, 32), 32)
            wide = xv[at, :].astype(jnp.float32)
            scale = lax.rsqrt(jnp.mean(wide * wide, axis=-1, keepdims=True) + 1e-6)
            out = (wide * scale * gain_ref[...].astype(jnp.float32)[None]).astype(jnp.bfloat16)
            for h in range(HEADS):
                lhs[0, h, at, :] = out[:, h * HEAD : (h + 1) * HEAD]

        _times(4, rows)

    def kv_project(which):
        if which == 0:
            for q in range(4):
                pltpu.make_async_copy(own_kv(q), kv_all.at[z, r, q], l_sem.at[0]).start()
            got(kv_all.at[z, r], l_sem.at[0])
            for k in range(4):
                handed(KV, z if k == 0 else source(k))

        def loop(n, _):
            total = acc[which]
            for half in range(2):
                w = kv_all[lax.div(n, 2), lax.rem(n, 2), 2 * half + which]
                total += _dot(lhs[0, 2 * n + half], w)
            acc[which] = total

        acc[which] = jnp.zeros((OWN, HEAD), jnp.float32)
        _times(8, loop, 2)
        if which == 0:
            ks[sp] = _turn(acc[which].astype(jnp.bfloat16).astype(jnp.float32), cos_ref[...], sin_ref[...])
        else:
            vts[sp, _top(HEAD), :] = acc[which].T.astype(jnp.bfloat16)
            for i in range(8):
                vts[i, pl.ds(HEAD, 16), :] = jnp.ones((16, OWN), jnp.bfloat16)

    def load(t, k):
        b = k % 2
        if k:
            s = source(k)
            handed(t, s)
            pltpu.make_async_copy(w_all.at[t, s], wt.at[b], l_sem.at[b]).start()
        else:
            handed(t, z)
            pltpu.make_async_copy(w_all.at[t, z, other], wt.at[b, other], l_sem.at[b]).start()

            def go(ref, c):
                for q in range(4):
                    pltpu.make_async_copy(columns(ref, q, c), wt.at[b, r, q], l_sem.at[b]).start()

            @pl.when(t < CHUNKS)
            def _():
                go(wq, t)

            @pl.when(t >= CHUNKS)
            def _():
                go(wo, t - CHUNKS)

    def mm(t, k):
        b = k % 2
        got(wt.at[b], l_sem.at[b])
        s = source(k) if k else z
        m = lax.div(t, CHUNKS)

        def one(q, _):
            total = None
            for rr in range(2):
                for half in range(2):
                    d = _dot(lhs[m, 4 * s + 2 * rr + half], wt[b, rr, q, pl.ds(half * 256, 256), :])
                    total = d if total is None else total + d
            acc[q] = total if k == 0 else acc[q] + total

        _times(4, one, 4)

    def quarter(t, k, q):
        s, m, totals = source(k), t // CHUNKS, []
        for rows in (_top(OWN // 2), pl.ds(OWN // 2, OWN // 2)):
            total = None
            for rr in range(2):
                for i in range(2):
                    d = _dot(lhs[m, 4 * s + 2 * rr + i, rows, :], wt[k % 2, rr, q, pl.ds(i * 256, 256), :])
                    total = d if total is None else total + d
            totals.append(total)
        acc[q] += jnp.concatenate(totals, axis=0)
        put(t, q)

    def put(t, q):
        at = pl.ds(pl.multiple_of((q * CHUNKS + t - CHUNKS) * HEAD, HEAD), HEAD)
        y_ref[:, at] = (xv[:, at].astype(jnp.float32) + acc[q]).astype(jnp.bfloat16)

    def finish(t):
        @pl.when(t < CHUNKS)
        def _():
            def one(q, _):
                v = acc[q].astype(jnp.bfloat16).astype(jnp.float32)
                qs[q * CHUNKS + t] = _turn(v, cos_ref[...], sin_ref[...])

            _times(4, one)

        @pl.when(t >= CHUNKS)
        def _():
            _times(4, lambda q, _: put(t, q))

    def attend(n, near):
        e = HEAD**-0.5 * LOG2E
        heads = []
        for i in range(GROUP):
            at = n * GROUP + i
            heads.append(lax.rem(at, 4) * CHUNKS + lax.div(at, 4))
        if near:
            for h in heads:
                top_s[h] = jnp.full((1, OWN), NEG, jnp.float32)
                mix_s[h] = jnp.zeros((HEAD + 8, OWN), jnp.float32)

        def block(j, n, masked):
            keys = ks[pl.ds(j, n)].reshape(n * OWN, HEAD)
            scores = [_dot(keys, qs[h], 1, 1) for h in heads]
            weights, keeps = [], []
            for h, s in zip(heads, scores):
                if masked:
                    key = lax.broadcasted_iota(jnp.int32, (OWN, OWN), 0)
                    own = jnp.where(lax.broadcasted_iota(jnp.int32, (OWN, OWN), 1) >= key, s[(n - 1) * OWN :], HIDDEN)
                    s = jnp.concatenate([s[: (n - 1) * OWN], own], axis=0) if n > 1 else own
                old = top_s[h]
                top = jnp.maximum(old, s.max(axis=0, keepdims=True))
                top_s[h] = top
                weights.append(jnp.exp2((s - top) * e).astype(jnp.bfloat16))
                keeps.append(jnp.exp2((old - top) * e))
            values = [vts[j + i, _top(HEAD + 8), :] for i in range(n)]
            for h, w, keep in zip(heads, weights, keeps):
                total = mix_s[h] * keep
                for i in range(n):
                    total += _dot(values[i], w[i * OWN : (i + 1) * OWN])
                mix_s[h] = total

        far = jnp.maximum(z - 1, 0)
        if near:
            pl.when(z > 0)(lambda: block(2 * (z - 1), 2, False))
            pl.when(r == 0)(lambda: block(sp, 1, True))
            pl.when(r == 1)(lambda: block(sp - 1, 2, True))
        else:
            _times(far, lambda j, _: block(2 * j, 2, False))
            for h in heads:
                lhs[1, h] = (mix_s[h, _top(HEAD), :] * (1 / mix_s[h, pl.ds(HEAD, 1), :])).T.astype(jnp.bfloat16)

    barrier = pltpu.get_barrier_semaphore()
    for dev in (DEV_IN, DEV_X, DEV_Y, DEV_D):
        pl.semaphore_signal(barrier, inc=1, device_id=dev, device_id_type=MESH)

    @pl.when(inner)
    def _():
        pl.semaphore_signal(barrier, inc=1, device_id=DEV_OUT, device_id_type=MESH)

    @pl.when(inner)
    def _():
        pl.semaphore_wait(barrier, 5)

    @pl.when(outer)
    def _():
        pl.semaphore_wait(barrier, 4)

    LAST = KV - 1

    def guarded(t, low, high, fn):
        if isinstance(t, int):
            if low <= t <= high:
                fn()
        else:
            pl.when((t >= low) & (t <= high))(fn)

    def in_round(t, n, fn):
        pl.when(t == n)(fn)

    def shifted(stage, t, k, by, but=None):
        at = k - 1 + by
        dt, kk = at // 3, at % 3 + 1
        if isinstance(t, int):
            if 0 <= t + dt <= LAST:
                stage(t + dt, kk)
        elif dt == 0 and but and kk in but[1]:
            pl.when(t != but[0])(lambda: stage(t, kk))
        elif dt == 0:
            stage(t, kk)
        else:
            pl.when((t + dt >= 0) & (t + dt <= LAST))(lambda: stage(t + dt, kk))

    send_own_kv()
    pltpu.make_async_copy(x_hbm, xv, x_sem.at[0]).start()
    pltpu.make_async_copy(gain_hbm, gain_ref, x_sem.at[1]).start()
    pltpu.make_async_copy(rate_hbm, rate_ref, x_sem.at[2]).start()
    send_own(0)
    stage0(KV, 1)
    stage1(KV, 1)
    got(xv, x_sem.at[0])
    got(gain_ref, x_sem.at[1])
    got(rate_ref, x_sem.at[2])
    norm(0)
    stage0(0, 1)
    stage1(0, 1)
    stage0(KV, 2)
    stage2(KV, 1)
    stage0(KV, 3)
    stage1(KV, 2)
    norm(1)
    stage0(0, 2)
    stage1(KV, 3)
    stage3(KV, 1)
    stage2(KV, 2)
    stage0(0, 3)
    stage1(0, 2)
    send_own(1)
    norm(2)
    stage2(KV, 3)
    stage3(KV, 2)
    norm(3)
    tables()

    def whole(t):
        for k in range(1, 4):
            load(t, k)
            mm(t, k - 1)
        load(t + 1, 0)
        mm(t, 3)
        finish(t)

    def _all(fns):
        for fn in fns:
            fn()

    def round_(t, _):
        pl.when(outer & (t < LAST - 1))(lambda: send_own(t + 2))
        before = t - 1
        early = lambda *fns: guarded(t, 1, CHUNKS, lambda: _all(fns))

        def ticks(k, mid):
            shifted(stage0, t, k, A0)
            shifted(stage1, t, k, 0, (0, (1, 2, 3)))
            mid[0]()
            shifted(stage2, t, k, -A2)
            mid[1]()
            shifted(stage3, t, k, -A3)
            mid[2]()

        def near(i):
            guarded(t, 2, 5, lambda: attend(2 * (t - 2) + i, True))

        def far(i, low=4):
            guarded(t, low, 6, lambda: attend(3 * (t - 4) + i, False))

        def nothing():
            pass

        def mid1():
            early(lambda: load(before, 1), lambda: mm(before, 0))
            in_round(t, 7, lambda: whole(5))

        def mid2():
            in_round(t, 2, lambda: kv_handed((0, 1)))
            near(0)

        def mid4():
            in_round(t, 4, lambda: kv_take(3))
            early(lambda: load(before, 2), lambda: mm(before, 1))

        def mid5():
            in_round(t, 0, lambda: _all((lambda: stage1(0, 3), lambda: stage3(KV, 3))))
            near(1)
            in_round(t, 4, lambda: kv_handed((2, 3)))

        def mid6():
            in_round(t, 0, lambda: kv_project(0))
            far(0)
            in_round(t, 7, lambda: whole(6))

        def mid7():
            in_round(t, 1, lambda: pl.when(z < 3)(lambda: kv_take(1)))
            in_round(t, 2, lambda: pl.when(z < 3)(lambda: kv_take(2)))
            in_round(t, 3, lambda: pl.when(z == 3)(lambda: kv_take(2)))
            early(lambda: load(before, 3), lambda: mm(before, 2))
            in_round(t, 6, lambda: load(4, 0))

        def mid8():
            in_round(t, 0, lambda: kv_project(1))
            far(1)

        def mid9():
            early(lambda: mm(before, 3), lambda: finish(before))
            in_round(t, 0, lambda: kv_send(z, True))
            in_round(t, 6, lambda: whole(4))

        early(lambda: load(before, 0))
        in_round(t, 2, lambda: pl.when(z == 3)(lambda: kv_take(1)))
        ticks(1, (mid1, mid2, lambda: far(-1, 5)))
        ticks(2, (mid4, mid5, mid6))
        pl.when(inner & (t < LAST - 1))(lambda: send_own(t + 2))
        ticks(3, (mid7, mid8, mid9))

    _times(KV, round_)
    assert A3 == A2 + 1
    steps = [(stage, LAST + 1, k, -by) for k in range(1, 4) for stage, by in ((stage2, A2), (stage3, A3))]
    final = steps.index((stage3, LAST + 1, A3, -A3))
    assert final == 3
    load(LAST, 1)
    mm(LAST, 0)
    for step in steps[:final]:
        shifted(*step)
    mm(LAST, 1)
    load(LAST, 2)
    for step in steps[final:]:
        shifted(*step)
    s = source(3)
    pltpu.make_async_copy(w_all.at[LAST, s, r], wt.at[1, r], l_sem.at[1]).start()
    got(w_all.at[LAST, s, other, _top(4), _top(OWN - (OWN - 2 * BOTH) // 4)], recv_d.at[turn(LAST, 4), s])
    for q in (p, px, py):
        pltpu.make_async_copy(w_all.at[LAST, s, other, q], wt.at[1, other, q], x_sem.at[1]).start()
    mm(LAST, 2)
    got(wt.at[1, r], l_sem.at[1])
    got(wt.at[1, other, _top(3)], x_sem.at[1])
    quarter(LAST, 3, p)
    quarter(LAST, 3, px)
    got(w_all.at[LAST, s, other, pd, pl.ds(BOTH, OWN - 2 * BOTH)], recv_e.at[0])
    last = pltpu.make_async_copy(w_all.at[LAST, s, other, pd], wt.at[1, other, pd], l_sem.at[1])
    last.start()
    quarter(LAST, 3, py)
    last.wait()
    quarter(LAST, 3, pd)
    all_sent()
    kv_sent()


def solution(mesh):
    bf, f32 = jnp.bfloat16, jnp.float32
    any_, vmem = pl.BlockSpec(memory_space=pl.ANY), pl.BlockSpec(memory_space=pltpu.VMEM)
    dma = pltpu.SemaphoreType.DMA

    def step(x, gain, wq, wk, wv, wo):
        half = HEAD // 2
        rate = THETA ** (-np.arange(half, dtype=np.float32) / half)
        rate = jnp.asarray(rate, f32)[None]
        y, _ = pl.pallas_call(
            _kernel,
            in_specs=[any_] * 7,
            out_specs=[vmem, any_],
            out_shape=[pltpu.VMEM((OWN, D), bf), jax.ShapeDtypeStruct((KV, 4, 2, 4, OWN, HEAD), bf)],
            scratch_shapes=[
                pltpu.VMEM((D,), bf),
                pltpu.VMEM((1, HEAD // 2), f32),
                pltpu.VMEM((OWN, HEAD // 2), f32),
                pltpu.VMEM((OWN, HEAD // 2), f32),
                pltpu.VMEM((4, 2, 4, 256, HEAD), bf),
                pltpu.VMEM((OWN, D), bf),
                pltpu.VMEM((2, HEADS, OWN, HEAD), bf),
                pltpu.VMEM((HEADS, OWN, HEAD), bf),
                pltpu.VMEM((8, OWN, HEAD), bf),
                pltpu.VMEM((8, HEAD + 16, OWN), bf),
                pltpu.VMEM((4, OWN, HEAD), f32),
                pltpu.VMEM((2, 2, 4, OWN, HEAD), bf),
                pltpu.VMEM((HEADS, 1, OWN), f32),
                pltpu.VMEM((HEADS, HEAD + 8, OWN), f32),
                dma((5, 4)), *[dma((3, 4))] * 4, dma((5, 4)), dma((1,)),
                *[dma((3,))] * 7,
                *[dma((4,))] * 4,
                dma((2,)), dma((3,)),
            ],
            compiler_params=pltpu.CompilerParams(collective_id=0, has_side_effects=True, vmem_limit_bytes=57 * 2**20),
        )(x, gain, wq, wk, wv, wo, rate)
        return y

    tokens, whole = P(("dp", "sp"), None), P("sp", None)
    return jax.shard_map(
        step,
        mesh=mesh,
        in_specs=(tokens, P(None), whole, whole, whole, whole),
        out_specs=tokens,
        check_vma=False,
    )
```
